32 devices in a mesh: freq: 16 (over z, x, core), grid: 2 (over y).
Axes of the slice: x: 2, y: 2, z: 4, core: 2. Of those that a mesh axis runs over, the one named last changes fastest.
Arguments:
- cross_spectra: float32 [2, 32, 256, 256], P(None, None, 'freq', 'grid'), as said below
- sensor_modes: float32 [32, 96, 256], P('freq', None, 'grid'), may hold values from -0.375 to 0.375
- source_modes: float32 [32, 96, 256], P('freq', None, 'grid'), may hold values from -6 to 6
- wavenumber: float32 [32, 96], P('freq'), may hold values from 0.5 to 2
- attenuation: float32 [32, 96], P('freq'), may hold values from 0.002 to 0.03
- mode_counts: int32 [32], P('freq'), may hold values from 48 to 96
Outputs:
- bartlett_power: float32 [64, 256], P('freq', 'grid')
The draws below stay inside these ranges and needn't reach their ends.
Inputs may be any that keep to these rules, and one draw needn't show every extreme that they name: `cross_spectra`: each bin's matrix K_f is Hermitian and positive definite. Modes with index mode_counts[f] or more are left out in bin f.
All inputs are finite; a program needn't handle non-finite values.
Results may differ from the reference program's by a relative error of at most 0.0003.
Values sent between devices are 32-bit elements; how exact they have to be, the bound alone decides.
A program may use at most 128 MiB of HBM per device.

```python
import math
import jax
import jax.numpy as jnp
from jax import lax

SENSORS = 256
MODES = 96
RANGES = 64
BINS = 32
DEPTHS = 256


def sensor_table(key):
    base = jax.random.fold_in(key, 201)
    values = jnp.clip(jax.random.normal(base, (BINS, MODES, SENSORS), jnp.float32), -6.0, 6.0)
    return (values / math.sqrt(SENSORS)).astype(jnp.float32)


def source_table(key):
    base = jax.random.fold_in(key, 202)
    values = jnp.clip(jax.random.normal(base, (BINS, MODES, DEPTHS), jnp.float32), -6.0, 6.0)
    return values.astype(jnp.float32)


def wave_table(key):
    base = jax.random.fold_in(key, 203)
    values = jnp.exp(jax.random.uniform(base, (BINS, MODES), jnp.float32, math.log(0.5), math.log(2.0)))
    return jnp.clip(values, 0.5, 2.0).astype(jnp.float32)


def atten_table(key):
    base = jax.random.fold_in(key, 204)
    values = jnp.exp(jax.random.uniform(base, (BINS, MODES), jnp.float32, math.log(0.002), math.log(0.03)))
    return jnp.clip(values, 0.002, 0.03).astype(jnp.float32)


def draw_sensor_modes(key, part):
    return sensor_table(key)


def draw_source_modes(key, part):
    return source_table(key)


def draw_wavenumber(key, part):
    return wave_table(key)


def draw_attenuation(key, part):
    return atten_table(key)


def draw_cross_spectra(key, part):
    snapshots = SENSORS // 2
    planted = 3
    key_real, key_imag, key_gain, key_bin, key_range, key_depth, key_power = jax.random.split(jax.random.fold_in(key, 17), 7)
    sample_real = jax.random.normal(key_real, (BINS, SENSORS, snapshots), jnp.float32) * math.sqrt(0.5)
    sample_imag = jax.random.normal(key_imag, (BINS, SENSORS, snapshots), jnp.float32) * math.sqrt(0.5)
    sensor_gain = jnp.exp(jax.random.uniform(key_gain, (BINS, SENSORS), jnp.float32, math.log(0.5), math.log(2.0)))
    bin_gain = jnp.exp(jax.random.uniform(key_bin, (BINS,), jnp.float32, math.log(0.3), math.log(3.0)))
    noise_real = (jnp.einsum('bis,bjs->bij', sample_real, sample_real) + jnp.einsum('bis,bjs->bij', sample_imag, sample_imag)) / snapshots
    noise_real = noise_real + jnp.eye(SENSORS, dtype=jnp.float32)[None]
    noise_imag = (jnp.einsum('bis,bjs->bij', sample_imag, sample_real) - jnp.einsum('bis,bjs->bij', sample_real, sample_imag)) / snapshots
    gain_outer = sensor_gain[:, :, None] * sensor_gain[:, None, :]
    noise_real = noise_real * gain_outer
    noise_imag = noise_imag * gain_outer
    shapes = sensor_table(key)
    sources = source_table(key)
    waves = wave_table(key)
    damping = atten_table(key)
    cell_range = jax.random.randint(key_range, (planted,), 0, RANGES)
    cell_depth = jax.random.randint(key_depth, (planted,), 0, DEPTHS)
    radius = 1.0 + cell_range.astype(jnp.float32)
    phase = waves[:, :, None] * radius[None, None, :]
    magnitude = jnp.exp(-damping[:, :, None] * radius[None, None, :]) / jnp.sqrt(phase)
    depth_shape = jnp.take(sources, cell_depth, axis=2)
    coef_real = magnitude * jnp.cos(phase) * depth_shape
    coef_imag = magnitude * jnp.sin(phase) * depth_shape
    steer_real = jnp.einsum('bmi,bmp->bpi', shapes, coef_real)
    steer_imag = jnp.einsum('bmi,bmp->bpi', shapes, coef_imag)
    length = jnp.sqrt(jnp.sum(steer_real * steer_real + steer_imag * steer_imag, axis=2, keepdims=True))
    unit_real = steer_real / length
    unit_imag = steer_imag / length
    noise_level = 2.0 * jnp.mean(sensor_gain * sensor_gain, axis=1)
    strength = jnp.exp(jax.random.uniform(key_power, (BINS, planted), jnp.float32, 0.0, math.log(10.0))) * noise_level[:, None]
    signal_real = jnp.einsum('bp,bpi,bpj->bij', strength, unit_real, unit_real) + jnp.einsum('bp,bpi,bpj->bij', strength, unit_imag, unit_imag)
    signal_imag = jnp.einsum('bp,bpi,bpj->bij', strength, unit_imag, unit_real) - jnp.einsum('bp,bpi,bpj->bij', strength, unit_real, unit_imag)
    real_part = (noise_real + signal_real) * bin_gain[:, None, None]
    imag_part = (noise_imag + signal_imag) * bin_gain[:, None, None]
    return jnp.stack([real_part, imag_part]).astype(jnp.float32)


def set_ends(result, stream_key, smallest, high):
    extent = result.shape
    index_at = [jax.random.randint(jax.random.fold_in(stream_key, axis), (), 0, extent[axis]) for axis in range(len(extent))]
    result = result.at[tuple(index_at)].set(smallest)
    longest = extent.index(max(extent))
    index_at[longest] = (index_at[longest] + 1) % extent[longest]
    return result.at[tuple(index_at)].set(high)


def setup_inputs(seed: int = 0) -> dict:
    keys = jax.random.split(jax.random.key(seed), 7)
    cross_spectra = draw_cross_spectra(jax.random.fold_in(keys[6], 71), 0)
    sensor_modes = draw_sensor_modes(jax.random.fold_in(keys[6], 71), 0)
    source_modes = draw_source_modes(jax.random.fold_in(keys[6], 71), 0)
    wavenumber = draw_wavenumber(jax.random.fold_in(keys[6], 71), 0)
    attenuation = draw_attenuation(jax.random.fold_in(keys[6], 71), 0)
    mode_counts = set_ends(jax.random.randint(keys[5], (BINS,), MODES // 2, MODES + 1), jax.random.fold_in(keys[5], 1), MODES // 2, MODES).astype(jnp.int32)
    return dict(cross_spectra=cross_spectra, sensor_modes=sensor_modes, source_modes=source_modes, wavenumber=wavenumber, attenuation=attenuation, mode_counts=mode_counts)


HIGH = lax.Precision.HIGHEST

def replica_terms(wave_row, atten_row, count, source_row, ranges):
    phase = wave_row[:, None] * ranges[None, :]
    magnitude = jnp.exp(-atten_row[:, None] * ranges[None, :]) / jnp.sqrt(phase)
    keep = (jnp.arange(source_row.shape[0], dtype=jnp.int32) < count).astype(jnp.float32)
    hankel_real = magnitude * jnp.cos(phase) * keep[:, None]
    hankel_imag = magnitude * jnp.sin(phase) * keep[:, None]
    coef_real = hankel_real[:, :, None] * source_row[:, None, :]
    coef_imag = hankel_imag[:, :, None] * source_row[:, None, :]
    return (coef_real, coef_imag)

def reference(cross_spectra, sensor_modes, source_modes, wavenumber, attenuation, mode_counts):
    ranges = 1.0 + jnp.arange(RANGES, dtype=jnp.float32)

    def one_bin(total, bin_index):
        spectra = cross_spectra[:, bin_index]
        shapes = sensor_modes[bin_index]
        product = jnp.einsum('cij,mj->cim', spectra, shapes, precision=HIGH)
        projected = jnp.einsum('mi,cin->cmn', shapes, product, precision=HIGH)
        gram = jnp.einsum('mi,ni->mn', shapes, shapes, precision=HIGH)
        coef_real, coef_imag = replica_terms(wavenumber[bin_index], attenuation[bin_index], mode_counts[bin_index], source_modes[bin_index], ranges)
        image_real = jnp.einsum('mn,nrz->mrz', projected[0], coef_real, precision=HIGH) - jnp.einsum('mn,nrz->mrz', projected[1], coef_imag, precision=HIGH)
        image_imag = jnp.einsum('mn,nrz->mrz', projected[1], coef_real, precision=HIGH) + jnp.einsum('mn,nrz->mrz', projected[0], coef_imag, precision=HIGH)
        numer = lax.optimization_barrier(jnp.sum(coef_real * image_real + coef_imag * image_imag, axis=0))
        gram_real = jnp.einsum('mn,nrz->mrz', gram, coef_real, precision=HIGH)
        gram_imag = jnp.einsum('mn,nrz->mrz', gram, coef_imag, precision=HIGH)
        denom = lax.optimization_barrier(jnp.sum(coef_real * gram_real + coef_imag * gram_imag, axis=0))
        return (total + numer / denom, None)
    total, unused = lax.scan(one_bin, jnp.zeros((RANGES, DEPTHS), jnp.float32), jnp.arange(BINS, dtype=jnp.int32))
    return total / BINS
```

```python
import functools

import jax
import jax.numpy as jnp
from jax import lax
from jax.experimental import pallas as pl
from jax.experimental.pallas import tpu as pltpu
from jax.sharding import PartitionSpec as P

RANGES = 64
BLOCK = 8
STEP = 8
LANES = 128

HIGH = lax.Precision.HIGHEST
MESH = pl.DeviceIdType.MESH
NT = (((1,), (1,)), ((), ()))
NN = (((1,), (0,)), ((), ()))


def split(value):
    high = value.astype(jnp.bfloat16)
    return high, (value - high.astype(jnp.float32)).astype(jnp.bfloat16)


def product(left, right, dims):
    return lax.dot_general(left, right, dims, preferred_element_type=jnp.float32)


def kernel(
    nf, ng,
    spectra_hbm, sensor_hbm, source_hbm, wave_hbm, atten_hbm, counts_hbm,
    out_ref,
    wave_ref, atten_ref, counts_ref, small_sem,
    raw, outgoing, table, shapes, sources, shapes_wide, halves, weight, rows_scr, cols_scr, row_in,
    u_scr, v_scr, lhs, denom, power, parts,
    raw_sem, own_sem, mode_send, mode_recv, send_sem, recv_sem, part_send, part_recv,
):
    devices = nf * ng
    bins = outgoing.shape[0]
    nb = bins // devices
    row_count, col_count = raw.shape[2], raw.shape[3]
    modes = shapes.shape[2]
    ranges = u_scr.shape[1]
    share = ranges // nf
    depth_here = sources.shape[3]
    my_f, my_g = lax.axis_index("freq"), lax.axis_index("grid")
    me = my_f * ng + my_g

    raw_copy = pltpu.make_async_copy(spectra_hbm, raw, raw_sem)
    raw_copy.start()
    small = [
        pltpu.make_async_copy(hbm, here, small_sem.at[i])
        for i, (hbm, here) in enumerate(
            ((wave_hbm, wave_ref), (atten_hbm, atten_ref), (counts_hbm, counts_ref))
        )
    ]
    for copy in small:
        copy.start()
    own = pl.ds(my_g * nb, nb)
    own_shapes = pltpu.make_async_copy(sensor_hbm.at[own], shapes.at[my_g], own_sem.at[0])
    own_sources = pltpu.make_async_copy(source_hbm.at[own], sources.at[my_g], own_sem.at[1])
    own_shapes.start()
    own_sources.start()

    barrier = pltpu.get_barrier_semaphore()

    def greet(k, carry):
        peer = lax.rem(me + k, devices)
        pl.semaphore_signal(
            barrier, inc=1, device_id=(peer // ng, lax.rem(peer, ng)), device_id_type=MESH
        )
        return carry

    lax.fori_loop(1, devices, greet, 0)

    raw_copy.wait()
    for copy in small:
        copy.wait()
    outgoing[...] = raw[0] + raw[1]
    my_rows = pl.ds(pl.multiple_of(my_f * row_count, row_count), row_count)
    for b in range(nb):
        table[my_g, b, my_rows, :] = outgoing[me * nb + b]

    pl.semaphore_wait(barrier, devices - 1)

    def mode_copies(k):
        peer = lax.rem(my_g + k, ng)
        theirs = pl.ds(peer * nb, nb)
        return [
            pltpu.make_async_remote_copy(
                src_ref=hbm.at[theirs],
                dst_ref=here.at[my_g],
                send_sem=mode_send.at[i, k],
                recv_sem=mode_recv.at[i, k],
                device_id=(my_f, peer),
                device_id_type=MESH,
            )
            for i, (hbm, here) in enumerate(((sensor_hbm, shapes), (source_hbm, sources)))
        ]

    for k in range(1, ng):
        for copy in mode_copies(k):
            copy.start()

    def piece(k):
        peer = lax.rem(me + k, devices)
        return pltpu.make_async_remote_copy(
            src_ref=outgoing.at[pl.ds(peer * nb, nb)],
            dst_ref=table.at[my_g, :, my_rows, :],
            send_sem=send_sem,
            recv_sem=recv_sem,
            device_id=(peer // ng, lax.rem(peer, ng)),
            device_id_type=MESH,
        )

    def send_piece(k, carry):
        piece(k).start()
        return carry

    lax.fori_loop(1, devices, lambda k, c: send_piece(devices - k, c), 0)

    for b in range(nb):
        row = my_g * nb + b
        row_in[...] = jnp.ones_like(row_in)
        row_in[0:1, 0:modes] = wave_ref[pl.ds(row, 1), :]
        row_in[1:2, 0:modes] = atten_ref[pl.ds(row, 1), :]
        radius = 1.0 + lax.broadcasted_iota(jnp.int32, (ranges, LANES), 0).astype(jnp.float32)
        lane = lax.broadcasted_iota(jnp.int32, (ranges, LANES), 1)
        phase = radius * row_in[0:1, :]
        magnitude = jnp.exp(-row_in[1:2, :] * radius) / jnp.sqrt(phase)
        magnitude = jnp.where(lane < counts_ref[row], magnitude, 0.0)
        filler = jnp.zeros((LANES - ranges, LANES), jnp.float32)
        for i, factor in enumerate((magnitude * jnp.cos(phase), magnitude * jnp.sin(phase))):
            rows_scr[b, i] = factor
            turned = jnp.concatenate([factor, filler], 0).T
            for blk in range(ranges // BLOCK):
                cols_scr[b, i, blk] = turned[0:modes, blk * BLOCK : (blk + 1) * BLOCK]

    for b in range(nb):

        def pair_block(blk, carry):
            first = pl.multiple_of(blk * BLOCK, BLOCK)
            row_real = rows_scr[b, 0, pl.ds(first, BLOCK), :]
            row_imag = rows_scr[b, 1, pl.ds(first, BLOCK), :]
            col_real, col_imag = cols_scr[b, 0, blk], cols_scr[b, 1, blk]
            for k in range(BLOCK):
                nr, ni = row_real[k : k + 1, :], row_imag[k : k + 1, :]
                mr = jnp.broadcast_to(col_real[:, k : k + 1], (modes, LANES))
                mi = jnp.broadcast_to(col_imag[:, k : k + 1], (modes, LANES))
                u_scr[b, first + k] = mr * nr + mi * ni
                v_scr[b, first + k] = mr * ni - mi * nr
            return carry

        lax.fori_loop(0, ranges // BLOCK, pair_block, 0)

    own_shapes.wait()
    own_sources.wait()
    for k in range(1, ng):
        for copy in mode_copies(k):
            copy.wait_recv()

    shapes_wide[...] = jnp.zeros_like(shapes_wide)
    halves[...] = jnp.zeros_like(halves)
    for b in range(nb):
        for g in range(ng):
            shapes_wide[b, 0:modes, g * col_count : (g + 1) * col_count] = shapes[g, b]
            exact = sources[g, b]
            rounded = exact.astype(jnp.bfloat16)
            at = slice(g * depth_here, (g + 1) * depth_here)
            halves[b, 0:modes, at] = rounded
            halves[b, LANES : LANES + modes, at] = rounded
            weight[b, :, at] = 2.0 * exact - rounded.astype(jnp.float32)

    def put(i, k, block):
        high = block.astype(jnp.bfloat16)
        low = (block - high.astype(jnp.float32)).astype(jnp.bfloat16)
        lhs[i, k * modes : (k + 1) * modes, 0:LANES] = high
        lhs[i, k * modes : (k + 1) * modes, LANES : 2 * LANES] = low

    def forms(i, b):
        image = jnp.dot(lhs[i], halves[b], preferred_element_type=jnp.float32)
        image = image.reshape(BLOCK, modes, image.shape[1]) * weight[b][None]
        return jnp.sum(image, axis=1)

    for b in range(nb):
        wide = shapes_wide[b]
        gram = lax.dot_general(
            wide[0:modes], wide, NT, precision=HIGH, preferred_element_type=jnp.float32
        )

        def denom_step(step, carry):
            for i in range(STEP):
                first = pl.multiple_of((step * STEP + i) * BLOCK, BLOCK)
                for k in range(BLOCK):
                    put(i, k, gram * u_scr[b, first + k])
                denom[b, pl.ds(first, BLOCK), :] = forms(i, b) * float(bins)
            return carry

        lax.fori_loop(0, ranges // BLOCK // STEP, denom_step, 0)

    def part(peer, slot):
        peer_f, peer_g = peer // ng, lax.rem(peer, ng)
        return pltpu.make_async_remote_copy(
            src_ref=power.at[peer_g, peer_f],
            dst_ref=parts.at[slot],
            send_sem=part_send,
            recv_sem=part_recv,
            device_id=(peer_f, peer_g),
            device_id_type=MESH,
        )

    blocks = ranges // BLOCK
    owners = BLOCK // share
    low = 1 - (my_f // owners * 2) // blocks

    def block_at(n):
        return lax.rem(my_f // owners + (1 - 2 * low) * (n + 1) + blocks, blocks)

    def send_block(n):
        for t in range(owners):
            for g in range(ng):
                part((block_at(n) * owners + t) * ng + g, me).start()

    def take_piece(k, carry):
        piece(k).wait_recv()
        return carry

    many = outgoing.at[pl.ds(0, (devices - 1) * nb)]
    most = parts.at[pl.ds(0, devices - 1)]
    def settle(ref, sem):
        pltpu.make_async_copy(ref, ref, sem).wait()
    settle(many, recv_sem)

    for b in range(nb):
        wide = shapes_wide[b]
        whole = jnp.concatenate([table[g, b] for g in range(ng)], axis=1)
        left_high, left_low = split(wide)
        mid_high, mid_low = split(whole)
        both = jnp.concatenate([left_high, left_low], 0)
        half = product(both, mid_high, NN)
        half = half[:LANES] + (half[LANES:] + product(left_high, mid_low, NN))
        half_high, half_low = split(half)
        both = jnp.concatenate([half_high, half_low], 0)
        full = product(both, left_high, NT)
        full = full[:LANES] + (full[LANES:] + product(half_high, left_low, NT))
        turned = full.T
        even = (0.5 * (full + turned))[0:modes]
        odd = (0.5 * (full - turned))[0:modes]

        def numer_step(step, carry):
            for i in range(STEP):
                blk = block_at(step * STEP + i)
                first = pl.multiple_of(blk * BLOCK, BLOCK)
                for k in range(BLOCK):
                    put(i, k, even * u_scr[b, first + k] - odd * v_scr[b, first + k])
                score = forms(i, b) / denom[b, pl.ds(first, BLOCK), :]
                for g in range(ng):
                    for t in range(owners):
                        at = slice(g * depth_here, (g + 1) * depth_here)
                        value = score[t * share : (t + 1) * share, at]
                        slot = blk * owners + t
                        if b == 0:
                            power[g, slot] = value
                        else:
                            power[g, slot] += value
                if b == nb - 1 and i > 0:
                    send_block(step * STEP + i - 1)
                elif b == nb - 1:

                    @pl.when(step > 0)
                    def _():
                        send_block(step * STEP - 1)

            return carry

        lax.fori_loop(0, ranges // BLOCK // STEP, numer_step, 0)

    def send_last(k, carry):
        peer = me // (owners * ng) * (owners * ng) + lax.rem(me + k, owners * ng)
        part(peer, me).start()
        return carry

    lax.fori_loop(1, owners * ng, send_last, 0)
    parts[me] = power[my_g, my_f]


    for k in range(1, ng):
        for copy in mode_copies(k):
            copy.wait_send()
    settle(many, send_sem)
    settle(most, part_send)
    settle(most, part_recv)
    out_ref[...] = jnp.sum(parts[...], axis=0)


def solution(mesh):
    nf, ng = mesh.shape["freq"], mesh.shape["grid"]
    devices = nf * ng

    def per_device(cross_spectra, sensor_modes, source_modes, wavenumber, attenuation, mode_counts):
        two, bins, rows, cols = cross_spectra.shape
        bins_here, modes, _ = sensor_modes.shape
        depth_here = source_modes.shape[2]
        nb = bins_here // ng
        ranges = RANGES // nf * nf
        share = ranges // nf
        f32, bf16 = jnp.float32, jnp.bfloat16
        dma = pltpu.SemaphoreType.DMA
        return pl.pallas_call(
            functools.partial(kernel, nf, ng),
            out_shape=jax.ShapeDtypeStruct((share, depth_here), f32),
            in_specs=[pl.BlockSpec(memory_space=pltpu.HBM)] * 6,
            out_specs=pl.BlockSpec(memory_space=pltpu.VMEM),
            scratch_shapes=[
                pltpu.VMEM(wavenumber.shape, f32), pltpu.VMEM(attenuation.shape, f32), pltpu.SMEM(mode_counts.shape, jnp.int32), pltpu.SemaphoreType.DMA((3,)),
                pltpu.VMEM((two, bins, rows, cols), f32),
                pltpu.VMEM((bins, rows, cols), f32),
                pltpu.VMEM((ng, nb, nf * rows, cols), f32),
                pltpu.VMEM((ng, nb, modes, cols), f32),
                pltpu.VMEM((ng, nb, modes, depth_here), f32),
                pltpu.VMEM((nb, LANES, ng * cols), f32),
                pltpu.VMEM((nb, 2 * LANES, ng * depth_here), bf16),
                pltpu.VMEM((nb, modes, ng * depth_here), f32),
                pltpu.VMEM((nb, 2, ranges, LANES), f32),
                pltpu.VMEM((nb, 2, ranges // BLOCK, modes, BLOCK), f32),
                pltpu.VMEM((8, LANES), f32),
                pltpu.VMEM((nb, ranges, modes, LANES), f32),
                pltpu.VMEM((nb, ranges, modes, LANES), f32),
                pltpu.VMEM((STEP, BLOCK * modes, 2 * LANES), bf16),
                pltpu.VMEM((nb, ranges, ng * depth_here), f32),
                pltpu.VMEM((ng, nf, share, depth_here), f32),
                pltpu.VMEM((devices, share, depth_here), f32),
                dma, dma((2,)), dma((2, ng)), dma((2, ng)),
                dma, dma, dma, dma,
            ],
            compiler_params=pltpu.CompilerParams(
                collective_id=0, has_side_effects=True, vmem_limit_bytes=24 * 1024 * 1024
            ),
        )(*[pltpu.with_memory_space_constraint(x, pltpu.HBM) for x in (cross_spectra, sensor_modes, source_modes, wavenumber, attenuation, mode_counts)])

    placed = (
        P(None, None, "freq", "grid"),
        P("freq", None, "grid"),
        P("freq", None, "grid"),
        P("freq", None),
        P("freq", None),
        P("freq"),
    )
    return jax.shard_map(
        per_device, mesh=mesh, in_specs=placed, out_specs=P("freq", "grid"), check_vma=False
    )
```

```python
import functools

import jax
import jax.numpy as jnp
from jax import lax
from jax.experimental import pallas as pl
from jax.experimental.pallas import tpu as pltpu
from jax.sharding import PartitionSpec as P

RANGES = 64
LANES = 128
CHUNK = 2
PLANES = 4

HIGH = lax.Precision.HIGHEST
MESH = pl.DeviceIdType.MESH
NT = (((1,), (1,)), ((), ()))
NN = (((1,), (0,)), ((), ()))


def split(value):
    high = value.astype(jnp.bfloat16)
    return high, (value - high.astype(jnp.float32)).astype(jnp.bfloat16)


def product(left, right, dims):
    return lax.dot_general(left, right, dims, preferred_element_type=jnp.float32)


def diagonals(square, modes):
    lane = lax.broadcasted_iota(jnp.int32, square.shape, 1)
    step = 1
    while step < modes:
        turned = pltpu.roll(square, modes - step, 0)
        square = jnp.where(lax.rem(lane // step, 2) == 1, turned, square)
        step *= 2
    return square


def kernel(
    nf, ng,
    spectra_hbm, sensor_hbm, source_hbm, wave_hbm, atten_hbm, counts_hbm,
    out_ref,
    wave, atten, counts, raw, plus, table, modes_out, shapes, sources, wide,
    first, second, right, rows, denom, power, parts,
    known, small_sem, raw_sem, own_sem, mode_send, mode_recv, send_sem, recv_sem, part_send, part_recv,
):
    devices = nf * ng
    bins, row_count, col_count = plus.shape
    nb = bins // devices
    modes = shapes.shape[2]
    half = modes // 2
    ranges = first.shape[2]
    share = ranges // nf
    depth_here = sources.shape[3]
    my_f, my_g = lax.axis_index("freq"), lax.axis_index("grid")
    me = my_f * ng + my_g

    barrier = pltpu.get_barrier_semaphore()
    span = nf // PLANES
    plane = my_f // span

    def flips(index, size):
        deltas, weight = [], 1
        while weight < size:
            deltas.append((1 - 2 * lax.rem(index // weight, 2)) * weight)
            weight *= 2
        return deltas

    flip_f, flip_g = flips(my_f, nf), flips(my_g, ng)

    def flipped(j):
        f, g = my_f, my_g
        for bit, delta in enumerate(flip_g + flip_f):
            if j >> bit & 1:
                if bit < len(flip_g):
                    g = g + delta
                else:
                    f = f + delta
        return f, g

    def signal(semaphore, f, g):
        pl.semaphore_signal(semaphore, inc=1, device_id=(f, g), device_id_type=MESH)

    def greet(f, carry):
        for g in range(ng):
            signal(barrier, nf + (plane + 1) * span - 1 - f, g)
        return carry

    lax.fori_loop((plane + 1) * span, nf, greet, 0)
    for j in range(span * ng - 1, 0, -1):
        signal(barrier, *flipped(j))

    raw_copy = pltpu.make_async_copy(spectra_hbm, raw, raw_sem)
    raw_copy.start()
    small = [
        pltpu.make_async_copy(hbm, here, small_sem.at[i])
        for i, (hbm, here) in enumerate(((wave_hbm, wave), (atten_hbm, atten), (counts_hbm, counts)))
    ]
    own = pl.ds(my_g * nb, nb)
    owned = [
        pltpu.make_async_copy(hbm, here, own_sem.at[i])
        for i, (hbm, here) in enumerate((
            (sensor_hbm, modes_out.at[0]),
            (source_hbm, modes_out.at[1]),
            (sensor_hbm.at[own], shapes.at[my_g]),
            (source_hbm.at[own], sources.at[my_g, :, 0:modes, :]),
            (source_hbm.at[own], sources.at[my_g, :, modes : 2 * modes, :]),
        ))
    ]
    for copy in small + owned:
        copy.start()

    raw_copy.wait()
    plus[...] = raw[0] + raw[1]
    my_rows = pl.ds(pl.multiple_of(my_f * row_count, row_count), row_count)
    for b in range(nb):
        table[my_g, b, my_rows, :] = plus[me * nb + b]

    for copy in owned:
        copy.wait()
    pl.semaphore_wait(barrier, (plane + 1) * span * ng - 1)
    for k in range(PLANES - 1, 0, -1):

        @pl.when(plane >= k)
        def _():
            signal(known.at[plane], my_f - k * span, my_g)

    def mode_copies(k):
        peer = lax.rem(my_g + k, ng)
        theirs = pl.ds(peer * nb, nb)
        places = (shapes.at[my_g], sources.at[my_g, :, 0:modes, :])
        return [
            pltpu.make_async_remote_copy(
                src_ref=modes_out.at[i, theirs],
                dst_ref=here,
                send_sem=mode_send.at[i, k - 1],
                recv_sem=mode_recv.at[i, k - 1],
                device_id=(my_f, peer),
                device_id_type=MESH,
            )
            for i, here in enumerate(places)
        ]

    for k in range(1, ng):
        for copy in mode_copies(k):
            copy.start()

    def piece(f, g):
        return pltpu.make_async_remote_copy(
            src_ref=plus.at[pl.ds((f * ng + g) * nb, nb)],
            dst_ref=table.at[my_g, :, my_rows, :],
            send_sem=send_sem,
            recv_sem=recv_sem,
            device_id=(f, g),
            device_id_type=MESH,
        )

    def send_plane(shift):
        for j in range(span * ng - 1, -1, -1):
            if j > 0 or shift is not None:
                f, g = flipped(j)
                piece(f if shift is None else f + shift, g).start()

    send_plane(None)
    for k in range(PLANES - 1, 0, -1):

        @pl.when(plane >= k)
        def _():
            send_plane(-k * span)

    for copy in small:
        copy.wait()
    radius = 1.0 + lax.broadcasted_iota(jnp.int32, (ranges, LANES), 0).astype(jnp.float32)
    lane = lax.broadcasted_iota(jnp.int32, (ranges, LANES), 1)
    for b in range(nb):
        row = my_g * nb + b
        rows[...] = jnp.ones_like(rows)
        rows[0:1, 0:modes] = wave[pl.ds(row, 1), :]
        rows[1:2, 0:modes] = atten[pl.ds(row, 1), :]
        phase = radius * rows[0:1, :]
        magnitude = jnp.exp(-rows[1:2, :] * radius) / jnp.sqrt(phase)
        magnitude = jnp.where(lane < jnp.minimum(counts[row], modes), magnitude, 0.0)
        first[b, 0] = magnitude * jnp.cos(phase)
        second[b, 0] = magnitude * jnp.sin(phase)

    for b in range(nb):
        real, imag = first[b, 0], second[b, 0]
        ahead = []
        for value in (real + imag, real - imag):
            ahead.append(jnp.where(lane < modes, value, pltpu.roll(value, modes, 1)))
        for d in range(half + 1):
            turned = []
            for value in ahead:
                if d > 0:
                    near = pltpu.roll(value, LANES - d, 1)
                    if modes - 1 + d >= LANES:
                        far = pltpu.roll(value, modes - d, 1)
                        near = jnp.where(lane < LANES - d, near, far)
                    value = near
                turned.append(value)
            total, gap = turned
            one = real * gap + imag * total
            two = real * total - imag * gap
            if d == 0 or 2 * d == modes:
                one, two = 0.5 * one, 0.5 * two
            first[b, d] = one
            second[b, d] = two

    for k in range(1, PLANES):

        @pl.when(plane + k < PLANES)
        def _():
            pl.semaphore_wait(known.at[plane + k], 1)
            send_plane(k * span)

    def lay_products(b, g):
        here = sources[g, b, 0:modes, :]
        none = jnp.zeros((LANES - modes, depth_here), jnp.bfloat16)
        for d in range(half + 1):
            pair = here * sources[g, b, d : d + modes, :]
            high, low = split(pair)
            slots = [(0, high), (1, high), (2, low)] if d == 0 else [(d + 2, high)]
            for slot, value in slots:
                right[b, g, slot * LANES : slot * LANES + modes, :] = value
                if modes < LANES:
                    right[b, g, slot * LANES + modes : (slot + 1) * LANES, :] = none

    for k in range(1, ng):
        for copy in mode_copies(k):
            copy.wait_recv()

    wide[...] = jnp.zeros_like(wide)
    for b in range(nb):
        for g in range(ng):
            wide[b, 0:modes, g * col_count : (g + 1) * col_count] = shapes[g, b]

            @pl.when(my_g != g)
            def _():
                sources[g, b, modes : 2 * modes, :] = sources[g, b, 0:modes, :]

            lay_products(b, g)

    def forms(b, lefts):
        slots = []
        for d in range(half + 1):
            value = lefts(d)
            high, low = split(value)
            slots += [high, low, high] if d == 0 else [high]
        totals = [None] * ng
        for k in range(0, len(slots), CHUNK):
            left = jnp.concatenate(slots[k : k + CHUNK], axis=1)
            end = k + len(slots[k : k + CHUNK])
            for n in range(ng):
                part = product(left, right[b, n, k * LANES : end * LANES, :], NN)
                totals[n] = part if totals[n] is None else totals[n] + part
        return jnp.concatenate(totals, axis=1)

    def spread(ref, d):
        return jnp.broadcast_to(ref[d : d + 1, :], (ranges, LANES))

    for b in range(nb):
        gram = lax.dot_general(
            wide[b, 0:modes], wide[b], NT, precision=HIGH, preferred_element_type=jnp.float32
        )
        rows[0:modes, :] = diagonals(gram, modes)
        value = forms(b, lambda d: spread(rows, d) * (first[b, d] + second[b, d]))
        denom[b] = value * float(bins)

    def settle(ref, sem):
        pltpu.make_async_copy(ref, ref, sem).wait()

    settle(plus.at[pl.ds(0, (devices - 1) * nb)], recv_sem)

    for b in range(nb):
        left_high, left_low = split(wide[b])
        whole = jnp.concatenate([table[g, b] for g in range(ng)], axis=1)
        mid_high, mid_low = split(whole)
        high, low = left_high[0:modes], left_low[0:modes]
        both = product(jnp.concatenate([high, low], 0), mid_high, NN)
        middle = both[:modes] + (both[modes:] + product(high, mid_low, NN))
        half_high, half_low = split(middle)
        both = product(jnp.concatenate([half_high, half_low], 0), left_high, NT)
        forward = both[:modes] + (both[modes:] + product(half_high, left_low, NT))
        square = jnp.zeros((LANES - modes, LANES), jnp.float32)
        backward = jnp.concatenate([forward, square], 0).T[0:modes]
        rows[0:modes, :] = diagonals(backward, modes)
        rows[LANES : LANES + modes, :] = diagonals(forward, modes)

        def left(d):
            return spread(rows, d) * first[b, d] + spread(rows, LANES + d) * second[b, d]

        score = forms(b, left) / denom[b]
        for g in range(ng):
            at = slice(g * depth_here, (g + 1) * depth_here)
            value = score[:, at].reshape(nf, share, depth_here)
            power[g] = value if b == 0 else power[g] + value

    def part(f, g):
        return pltpu.make_async_remote_copy(
            src_ref=power.at[g, f],
            dst_ref=parts.at[me],
            send_sem=part_send,
            recv_sem=part_recv,
            device_id=(f, g),
            device_id_type=MESH,
        )

    for j in range(devices - 1, 0, -1):
        part(*flipped(j)).start()
    parts[me] = power[my_g, my_f]

    for k in range(1, ng):
        for copy in mode_copies(k):
            copy.wait_send()

    settle(plus.at[pl.ds(0, (devices - 1) * nb)], send_sem)
    settle(parts.at[pl.ds(0, devices - 1)], part_send)
    settle(parts.at[pl.ds(0, devices - 1)], part_recv)
    out_ref[...] = jnp.sum(parts[...], axis=0)


def solution(mesh):
    nf, ng = mesh.shape["freq"], mesh.shape["grid"]
    devices = nf * ng

    def per_device(cross_spectra, sensor_modes, source_modes, wavenumber, attenuation, mode_counts):
        two, bins, rows, cols = cross_spectra.shape
        bins_here, modes, _ = sensor_modes.shape
        depth_here = source_modes.shape[2]
        nb = bins_here // ng
        ranges = RANGES // nf * nf
        share = ranges // nf
        slots = modes // 2 + 3
        f32, bf16 = jnp.float32, jnp.bfloat16
        dma = pltpu.SemaphoreType.DMA
        operands = (
            cross_spectra, sensor_modes, source_modes, wavenumber, attenuation, mode_counts
        )
        return pl.pallas_call(
            functools.partial(kernel, nf, ng),
            out_shape=jax.ShapeDtypeStruct((share, depth_here), f32),
            in_specs=[pl.BlockSpec(memory_space=pltpu.HBM)] * 6,
            out_specs=pl.BlockSpec(memory_space=pltpu.VMEM),
            scratch_shapes=[
                pltpu.VMEM((bins_here, modes), f32),
                pltpu.VMEM((bins_here, modes), f32),
                pltpu.SMEM((bins_here,), jnp.int32),
                pltpu.VMEM((two, bins, rows, cols), f32),
                pltpu.VMEM((bins, rows, cols), f32),
                pltpu.VMEM((ng, nb, nf * rows, cols), f32),
                pltpu.VMEM((2, bins_here, modes, cols), f32),
                pltpu.VMEM((ng, nb, modes, cols), f32),
                pltpu.VMEM((ng, nb, 2 * modes, depth_here), f32),
                pltpu.VMEM((nb, LANES, ng * cols), f32),
                pltpu.VMEM((nb, modes // 2 + 1, ranges, LANES), f32),
                pltpu.VMEM((nb, modes // 2 + 1, ranges, LANES), f32),
                pltpu.VMEM((nb, ng, slots * LANES, depth_here), bf16),
                pltpu.VMEM((2 * LANES, LANES), f32),
                pltpu.VMEM((nb, ranges, ng * depth_here), f32),
                pltpu.VMEM((ng, nf, share, depth_here), f32),
                pltpu.VMEM((devices, share, depth_here), f32),
                pltpu.SemaphoreType.REGULAR((PLANES,)),
                dma((3,)), dma, dma((5,)), dma((2, max(ng - 1, 1))), dma((2, max(ng - 1, 1))),
                dma, dma, dma, dma,
            ],
            compiler_params=pltpu.CompilerParams(
                collective_id=0, has_side_effects=True, vmem_limit_bytes=32 * 1024 * 1024
            ),
        )(*[pltpu.with_memory_space_constraint(x, pltpu.HBM) for x in operands])

    placed = (
        P(None, None, "freq", "grid"),
        P("freq", None, "grid"),
        P("freq", None, "grid"),
        P("freq", None),
        P("freq", None),
        P("freq"),
    )
    return jax.shard_map(
        per_device, mesh=mesh, in_specs=placed, out_specs=P("freq", "grid"), check_vma=False
    )
```

```python
import functools

import jax
import jax.numpy as jnp
from jax import lax
from jax.experimental import pallas as pl
from jax.experimental.pallas import tpu as pltpu
from jax.sharding import PartitionSpec as P

RANGES = 64
LANES = 128
CHUNK = 2
PLANES = 4

HIGH = lax.Precision.HIGHEST
MESH = pl.DeviceIdType.MESH
NT = (((1,), (1,)), ((), ()))
NN = (((1,), (0,)), ((), ()))


def split(value):
    high = value.astype(jnp.bfloat16)
    return high, (value - high.astype(jnp.float32)).astype(jnp.bfloat16)


def product(left, right, dims):
    return lax.dot_general(left, right, dims, preferred_element_type=jnp.float32)


def thrice(left, right, rows, dims):
    high, low = left[0][0:rows], left[1][0:rows]
    both = product(jnp.concatenate([high, low], 0), right[0], dims)
    return both[:rows] + (both[rows:] + product(high, right[1], dims))


def diagonals(square, modes):
    lane = lax.broadcasted_iota(jnp.int32, square.shape, 1)
    step = 1
    while step < modes:
        turned = pltpu.roll(square, modes - step, 0)
        square = jnp.where(lax.rem(lane // step, 2) == 1, turned, square)
        step *= 2
    return square


def kernel(
    nf, ng,
    spectra_hbm, sensor_hbm, source_hbm, wave_hbm, atten_hbm, counts_hbm,
    out_ref,
    wave, atten, counts, raw, plus, minus, table, mirror, relay, modes_out, shapes, sources,
    first, second, right, rows, denom, power, parts,
    known, small_sem, raw_sem, own_sem, mode_send, mode_recv, send_sem, recv_sem,
    relay_send, relay_recv, part_send, part_recv,
):
    devices = nf * ng
    nb, row_count, col_count = plus.shape[2:]
    paired = ng == 2
    per = nf // ng
    group = per * row_count
    modes = modes_out.shape[2]
    half = modes // 2
    ranges = first.shape[2]
    share = ranges // nf
    depth_here = sources.shape[3]
    my_f, my_g = lax.axis_index("freq"), lax.axis_index("grid")
    me = my_f * ng + my_g
    home = my_f // per
    crossed = home != my_g
    straight = home == my_g

    barrier = pltpu.get_barrier_semaphore()
    span = nf // PLANES
    plane = my_f // span

    def flips(index, size):
        deltas, weight = [], 1
        while weight < size:
            deltas.append((1 - 2 * lax.rem(index // weight, 2)) * weight)
            weight *= 2
        return deltas

    flip_f, flip_g = flips(my_f, nf), flips(my_g, ng)

    def flipped(j):
        f, g = my_f, my_g
        for bit, delta in enumerate(flip_g + flip_f):
            if j >> bit & 1:
                if bit < len(flip_g):
                    g = g + delta
                else:
                    f = f + delta
        return f, g

    def signal(semaphore, f, g):
        pl.semaphore_signal(semaphore, inc=1, device_id=(f, g), device_id_type=MESH)

    def greet(f, carry):
        for g in range(ng):
            signal(barrier, nf + (plane + 1) * span - 1 - f, g)
        return carry

    lax.fori_loop((plane + 1) * span, nf, greet, 0)
    for j in range(span * ng - 1, 0, -1):
        signal(barrier, *flipped(j))

    raw_copy = pltpu.make_async_copy(spectra_hbm, raw, raw_sem)
    raw_copy.start()
    small = [
        pltpu.make_async_copy(hbm, here, small_sem.at[i])
        for i, (hbm, here) in enumerate(((wave_hbm, wave), (atten_hbm, atten), (counts_hbm, counts)))
    ]
    own = pl.ds(my_g * nb, nb)
    owned = [
        pltpu.make_async_copy(hbm, here, own_sem.at[i])
        for i, (hbm, here) in enumerate((
            (sensor_hbm, modes_out.at[0]),
            (source_hbm, modes_out.at[1]),
            (sensor_hbm.at[own], shapes.at[my_g, :, 0:modes, :]),
            (source_hbm.at[own], sources.at[my_g, :, 0:modes, :]),
            (source_hbm.at[own], sources.at[my_g, :, modes : 2 * modes, :]),
        ))
    ]
    for copy in small + owned:
        copy.start()

    raw_copy.wait()
    plus[...] = (raw[0] + raw[1]).reshape(plus.shape)
    my_rows = pl.ds(pl.multiple_of(my_f * row_count, row_count), row_count)
    near_rows = pl.ds(pl.multiple_of(lax.rem(my_f, per) * row_count, row_count), row_count)
    for b in range(nb):
        table[my_g, b, my_rows, :] = plus[my_f, my_g, b]
    if paired:
        away = 1 - home
        away_rows = pl.ds(pl.multiple_of(away * group, group), group)

        @pl.when(straight)
        def _():
            mirror[...] = jnp.zeros_like(mirror)

        @pl.when(crossed)
        def _():
            table[home, :, away_rows, :] = jnp.zeros((nb, group, col_count), jnp.float32)
            minus[...] = (raw[0] - raw[1]).reshape(minus.shape)
            for b in range(nb):
                mirror[b, near_rows, :] = minus[my_f, my_g, b]

    if modes < LANES:
        shapes[:, :, modes:, :] = jnp.zeros((ng, nb, LANES - modes, col_count), jnp.float32)

    for copy in owned:
        copy.wait()
    pl.semaphore_wait(barrier, (plane + 1) * span * ng - 1)
    for k in range(PLANES - 1, 0, -1):

        @pl.when(plane >= k)
        def _():
            signal(known.at[plane], my_f - k * span, my_g)

    def mode_copies(k):
        peer = lax.rem(my_g + k, ng)
        theirs = pl.ds(peer * nb, nb)
        places = (shapes.at[my_g, :, 0:modes, :], sources.at[my_g, :, 0:modes, :])
        return [
            pltpu.make_async_remote_copy(
                src_ref=modes_out.at[i, theirs],
                dst_ref=here,
                send_sem=mode_send.at[i, k - 1],
                recv_sem=mode_recv.at[i, k - 1],
                device_id=(my_f, peer),
                device_id_type=MESH,
            )
            for i, here in enumerate(places)
        ]

    def copy_to(source, target, i, f, g):
        return pltpu.make_async_remote_copy(
            src_ref=source,
            dst_ref=target,
            send_sem=send_sem.at[i],
            recv_sem=recv_sem.at[i],
            device_id=(f, g),
            device_id_type=MESH,
        )

    last = away * (nf - span) if paired else 0

    def relay_copy():
        return pltpu.make_async_remote_copy(
            src_ref=plus.at[pl.ds(last, span), 1 - my_g],
            dst_ref=relay,
            send_sem=relay_send,
            recv_sem=relay_recv,
            device_id=(my_f, 1 - my_g),
            device_id_type=MESH,
        )

    def send_near(shift, start):
        peers = [(j, flipped(j)) for j in range(span * ng - 1, start - 1, -1)]
        for j, (f, g) in peers:
            f = f + shift
            copy_to(plus.at[f, g], table.at[my_g, :, my_rows, :], 0, f, g).start()
        if paired:

            @pl.when(crossed)
            def _():
                for j, (f, g) in peers:
                    if j % ng == 0:
                        f = f + shift
                        copy_to(minus.at[f, g], mirror.at[:, near_rows, :], 1, f, g).start()

    def send_far(shift, straight_only, crossed_only):
        ends = (my_f + shift) // span * span == last
        target = table.at[home, :, my_rows, :]

        def sends(source, js):
            for j in js:
                f, g = flipped(j)
                f = f + shift
                copy_to(source(f, g), target, 0, f, g).start()

        if not crossed_only:

            @pl.when(straight & jnp.logical_not(ends))
            def _():
                sends(lambda f, g: plus.at[f, g], range(span * ng - 1, -1, -1))

            @pl.when(straight & ends)
            def _():
                sends(lambda f, g: plus.at[f, g], range((span - 1) * ng, -1, -ng))

        if straight_only or not crossed_only:

            @pl.when(crossed)
            def _():
                for j in range((span - 1) * ng, -1, -ng):
                    f = flipped(j)[0] + shift
                    copy_to(plus.at[f, my_g], table.at[my_g, :, my_rows, :], 0, f, my_g).start()

        if not straight_only:

            @pl.when(crossed & ends)
            def _():
                sends(lambda f, g: relay.at[f - last], range((span - 1) * ng, -1, -ng))

    def send_plane(shift, **which):
        if not paired:
            send_near(shift, 0)
            return
        there = (my_f + shift) // per

        @pl.when(there == home)
        def _():
            send_near(shift, 0)

        @pl.when(there != home)
        def _():
            send_far(shift, **which)

    if paired:

        @pl.when(straight)
        def _():
            relay_copy().start()

    @pl.when(plane > 0)
    def _():
        for k in range(1, ng):
            for copy in mode_copies(k):
                copy.start()

    for copy in small:
        copy.wait()
    radius = 1.0 + lax.broadcasted_iota(jnp.int32, (ranges, LANES), 0).astype(jnp.float32)
    lane = lax.broadcasted_iota(jnp.int32, (ranges, LANES), 1)
    for b in range(nb):
        row = my_g * nb + b
        rows[...] = jnp.ones_like(rows)
        rows[0:1, 0:modes] = wave[pl.ds(row, 1), :]
        rows[1:2, 0:modes] = atten[pl.ds(row, 1), :]
        phase = radius * rows[0:1, :]
        magnitude = jnp.exp(-rows[1:2, :] * radius) / jnp.sqrt(phase)
        magnitude = jnp.where(lane < jnp.minimum(counts[row], modes), magnitude, 0.0)
        first[b, 0] = magnitude * jnp.cos(phase)
        second[b, 0] = magnitude * jnp.sin(phase)

    for b in range(nb):
        real, imag = first[b, 0], second[b, 0]
        ahead = []
        for value in (real + imag, real - imag):
            ahead.append(jnp.where(lane < modes, value, pltpu.roll(value, modes, 1)))
        for d in range(half + 1):
            turned = []
            for value in ahead:
                if d > 0:
                    near = pltpu.roll(value, LANES - d, 1)
                    if modes - 1 + d >= LANES:
                        far = pltpu.roll(value, modes - d, 1)
                        near = jnp.where(lane < LANES - d, near, far)
                    value = near
                turned.append(value)
            total, gap = turned
            one = real * gap + imag * total
            two = real * total - imag * gap
            if d == 0 or 2 * d == modes:
                one, two = 0.5 * one, 0.5 * two
            first[b, d] = one
            second[b, d] = two

    send_near(0, 1)
    for k in range(PLANES - 1, 0, -1):

        @pl.when(plane >= k)
        def _():
            send_plane(-k * span, straight_only=True, crossed_only=False)

    if paired:

        @pl.when(crossed & (plane >= PLANES // 2))
        def _():
            relay_copy().wait_recv()
            for k in range(PLANES // 2, PLANES):

                @pl.when(plane == k)
                def _():
                    send_far(-k * span, False, True)

    for k in range(1, PLANES):

        @pl.when(plane + k < PLANES)
        def _():
            pl.semaphore_wait(known.at[plane + k], 1)
            if paired:

                @pl.when(crossed & (plane < PLANES // 2) & (plane + k == PLANES - 1))
                def _():
                    relay_copy().wait_recv()

            send_plane(k * span, straight_only=False, crossed_only=False)

    @pl.when(plane == 0)
    def _():
        for k in range(1, ng):
            for copy in mode_copies(k):
                copy.start()

    def lay_products(b, g):
        here = sources[g, b, 0:modes, :]
        none = jnp.zeros((LANES - modes, depth_here), jnp.bfloat16)
        for d in range(half + 1):
            pair = here * sources[g, b, d : d + modes, :]
            high, low = split(pair)
            slots = [(0, high), (1, high), (2, low)] if d == 0 else [(d + 2, high)]
            for slot, value in slots:
                right[b, g, slot * LANES : slot * LANES + modes, :] = value
                if modes < LANES:
                    right[b, g, slot * LANES + modes : (slot + 1) * LANES, :] = none

    for k in range(1, ng):
        for copy in mode_copies(k):
            copy.wait_recv()

    for b in range(nb):
        for g in range(ng):
            @pl.when(my_g != g)
            def _():
                sources[g, b, modes : 2 * modes, :] = sources[g, b, 0:modes, :]

            lay_products(b, g)

    def forms(b, lefts):
        slots = []
        for d in range(half + 1):
            value = lefts(d)
            high, low = split(value)
            slots += [high, low, high] if d == 0 else [high]
        totals = [None] * ng
        for k in range(0, len(slots), CHUNK):
            left = jnp.concatenate(slots[k : k + CHUNK], axis=1)
            end = k + len(slots[k : k + CHUNK])
            for n in range(ng):
                part = product(left, right[b, n, k * LANES : end * LANES, :], NN)
                totals[n] = part if totals[n] is None else totals[n] + part
        return jnp.concatenate(totals, axis=1)

    def spread(ref, d):
        return jnp.broadcast_to(ref[d : d + 1, :], (ranges, LANES))

    for b in range(nb):
        wide = jnp.concatenate([shapes[g, b] for g in range(ng)], axis=1)
        gram = lax.dot_general(
            wide[0:modes], wide, NT, precision=HIGH, preferred_element_type=jnp.float32
        )
        rows[0:modes, :] = diagonals(gram, modes)
        value = forms(b, lambda d: spread(rows, d) * (first[b, d] + second[b, d]))
        denom[b] = value * float(devices * nb)

    def settle(ref, sem):
        pltpu.make_async_copy(ref, ref, sem).wait()

    def pieces(count):
        return raw.at[0, pl.ds(0, count * nb)]

    if paired:

        @pl.when(straight)
        def _():
            settle(pieces(devices - 1), recv_sem.at[0])

        @pl.when(crossed)
        def _():
            settle(pieces(nf + per - 1), recv_sem.at[0])
            settle(pieces(per - 1), recv_sem.at[1])

    else:
        settle(pieces(devices - 1), recv_sem.at[0])

    for b in range(nb):
        blocks = [split(shapes[g, b]) for g in range(ng)]
        left = [jnp.concatenate([block[i] for block in blocks], axis=1) for i in range(2)]
        whole = split(jnp.concatenate([table[g, b] for g in range(ng)], axis=1))
        both = thrice(split(thrice(left, whole, modes, NN)), left, modes, NT)
        square = jnp.zeros((LANES - modes, LANES), jnp.float32)
        forward, backward = both, jnp.concatenate([both, square], 0).T[0:modes]
        if paired:
            here, there = split(shapes[home, b]), split(shapes[away, b])
            across = thrice(split(thrice(here, split(mirror[b]), modes, NN)), there, modes, NT)
            backward = backward + across
            forward = forward + jnp.concatenate([across, square], 0).T[0:modes]
        rows[0:modes, :] = diagonals(backward, modes)
        rows[LANES : LANES + modes, :] = diagonals(forward, modes)

        def left(d):
            return spread(rows, d) * first[b, d] + spread(rows, LANES + d) * second[b, d]

        score = forms(b, left) / denom[b]
        for g in range(ng):
            at = slice(g * depth_here, (g + 1) * depth_here)
            value = score[:, at].reshape(nf, share, depth_here)
            power[g] = value if b == 0 else power[g] + value

    def part(f, g):
        return pltpu.make_async_remote_copy(
            src_ref=power.at[g, f],
            dst_ref=parts.at[me],
            send_sem=part_send,
            recv_sem=part_recv,
            device_id=(f, g),
            device_id_type=MESH,
        )

    for j in range(devices - 1, 0, -1):
        part(*flipped(j)).start()
    parts[me] = power[my_g, my_f]

    for k in range(1, ng):
        for copy in mode_copies(k):
            copy.wait_send()

    if paired:
        settle(pieces(nf - 1 + nf - span), send_sem.at[0])

        @pl.when(crossed)
        def _():
            settle(pieces(per - 1), send_sem.at[1])

        @pl.when(straight)
        def _():
            relay_copy().wait_send()

    else:
        settle(pieces(devices - 1), send_sem.at[0])

    settle(parts.at[pl.ds(0, devices - 1)], part_send)
    settle(parts.at[pl.ds(0, devices - 1)], part_recv)
    out_ref[...] = jnp.sum(parts[...], axis=0)


def solution(mesh):
    nf, ng = mesh.shape["freq"], mesh.shape["grid"]
    devices = nf * ng

    def per_device(cross_spectra, sensor_modes, source_modes, wavenumber, attenuation, mode_counts):
        two, bins, rows, cols = cross_spectra.shape
        bins_here, modes, _ = sensor_modes.shape
        depth_here = source_modes.shape[2]
        nb = bins_here // ng
        ranges = RANGES // nf * nf
        share = ranges // nf
        slots = modes // 2 + 3
        f32, bf16 = jnp.float32, jnp.bfloat16
        dma = pltpu.SemaphoreType.DMA
        operands = (
            cross_spectra, sensor_modes, source_modes, wavenumber, attenuation, mode_counts
        )
        return pl.pallas_call(
            functools.partial(kernel, nf, ng),
            out_shape=jax.ShapeDtypeStruct((share, depth_here), f32),
            in_specs=[pl.BlockSpec(memory_space=pltpu.HBM)] * 6,
            out_specs=pl.BlockSpec(memory_space=pltpu.VMEM),
            scratch_shapes=[
                pltpu.VMEM((bins_here, modes), f32),
                pltpu.VMEM((bins_here, modes), f32),
                pltpu.SMEM((bins_here,), jnp.int32),
                pltpu.VMEM((two, bins, rows, cols), f32),
                pltpu.VMEM((nf, ng, nb, rows, cols), f32),
                pltpu.VMEM((nf, ng, nb, rows, cols), f32),
                pltpu.VMEM((ng, nb, nf * rows, cols), f32),
                pltpu.VMEM((nb, nf // ng * rows, cols), f32),
                pltpu.VMEM((nf // PLANES, nb, rows, cols), f32),
                pltpu.VMEM((2, bins_here, modes, cols), f32),
                pltpu.VMEM((ng, nb, LANES, cols), f32),
                pltpu.VMEM((ng, nb, 2 * modes, depth_here), f32),
                pltpu.VMEM((nb, modes // 2 + 1, ranges, LANES), f32),
                pltpu.VMEM((nb, modes // 2 + 1, ranges, LANES), f32),
                pltpu.VMEM((nb, ng, slots * LANES, depth_here), bf16),
                pltpu.VMEM((2 * LANES, LANES), f32),
                pltpu.VMEM((nb, ranges, ng * depth_here), f32),
                pltpu.VMEM((ng, nf, share, depth_here), f32),
                pltpu.VMEM((devices, share, depth_here), f32),
                pltpu.SemaphoreType.REGULAR((PLANES,)),
                dma((3,)), dma, dma((5,)), dma((2, max(ng - 1, 1))), dma((2, max(ng - 1, 1))),
                dma((2,)), dma((2,)), dma, dma, dma, dma,
            ],
            compiler_params=pltpu.CompilerParams(
                collective_id=0, has_side_effects=True, vmem_limit_bytes=32 * 1024 * 1024
            ),
        )(*[pltpu.with_memory_space_constraint(x, pltpu.HBM) for x in operands])

    placed = (
        P(None, None, "freq", "grid"),
        P("freq", None, "grid"),
        P("freq", None, "grid"),
        P("freq", None),
        P("freq", None),
        P("freq"),
    )
    return jax.shard_map(
        per_device, mesh=mesh, in_specs=placed, out_specs=P("freq", "grid"), check_vma=False
    )
```

```python
import functools

import jax
import jax.numpy as jnp
from jax import lax
from jax.experimental import pallas as pl
from jax.experimental.pallas import tpu as pltpu
from jax.sharding import PartitionSpec as P

RANGES = 64
LANES = 128
CHUNK = 2
PLANES = 4

HIGH = lax.Precision.HIGHEST
MESH = pl.DeviceIdType.MESH
NT = (((1,), (1,)), ((), ()))
NN = (((1,), (0,)), ((), ()))


def split(value):
    high = value.astype(jnp.bfloat16)
    return high, (value - high.astype(jnp.float32)).astype(jnp.bfloat16)


def product(left, right, dims):
    return lax.dot_general(left, right, dims, preferred_element_type=jnp.float32)


def thrice(left, right, rows, dims):
    high, low = left[0][0:rows], left[1][0:rows]
    both = product(jnp.concatenate([high, low], 0), right[0], dims)
    return both[:rows] + (both[rows:] + product(high, right[1], dims))


def diagonals(square, modes):
    lane = lax.broadcasted_iota(jnp.int32, square.shape, 1)
    step = 1
    while step < modes:
        turned = pltpu.roll(square, modes - step, 0)
        square = jnp.where(lax.rem(lane // step, 2) == 1, turned, square)
        step *= 2
    return square


def kernel(
    nf, ng,
    spectra_hbm, sensor_hbm, source_hbm, wave_hbm, atten_hbm, counts_hbm,
    out_ref,
    wave, atten, counts, raw, plus, minus, table, mirror, relay, modes_out, shapes, sources,
    first, second, right, rows, denom, power, parts,
    known, small_sem, raw_sem, own_sem, mode_send, mode_recv, send_sem, recv_sem,
    relay_send, relay_recv, part_send, part_recv,
):
    devices = nf * ng
    nb, row_count, col_count = plus.shape[2:]
    paired = ng == 2
    per = nf // ng
    group = per * row_count
    modes = modes_out.shape[2]
    half = modes // 2
    ranges = first.shape[2]
    share = ranges // nf
    depth_here = sources.shape[3]
    my_f, my_g = lax.axis_index("freq"), lax.axis_index("grid")
    me = my_f * ng + my_g
    home = my_f // per
    crossed = home != my_g
    straight = home == my_g

    barrier = pltpu.get_barrier_semaphore()
    span = nf // PLANES
    plane = my_f // span

    def flips(index, size):
        deltas, weight = [], 1
        while weight < size:
            deltas.append((1 - 2 * lax.rem(index // weight, 2)) * weight)
            weight *= 2
        return deltas

    flip_f, flip_g = flips(my_f, nf), flips(my_g, ng)

    def flipped(j):
        f, g = my_f, my_g
        for bit, delta in enumerate(flip_g + flip_f):
            if j >> bit & 1:
                if bit < len(flip_g):
                    g = g + delta
                else:
                    f = f + delta
        return f, g

    def signal(semaphore, f, g):
        pl.semaphore_signal(semaphore, inc=1, device_id=(f, g), device_id_type=MESH)

    def greet(f, carry):
        for g in range(ng):
            signal(barrier, nf + (plane + 1) * span - 1 - f, g)
        return carry

    lax.fori_loop((plane + 1) * span, nf, greet, 0)
    for j in range(span * ng - 1, 0, -1):
        signal(barrier, *flipped(j))

    def settle(ref, sem):
        pltpu.make_async_copy(ref, ref, sem).wait()

    raw_copy = pltpu.make_async_copy(spectra_hbm, raw, raw_sem)
    raw_copy.start()
    small = [
        pltpu.make_async_copy(hbm, here, small_sem.at[i])
        for i, (hbm, here) in enumerate(((wave_hbm, wave), (atten_hbm, atten), (counts_hbm, counts)))
    ]
    own = pl.ds(my_g * nb, nb)
    owned = [
        pltpu.make_async_copy(hbm, here, own_sem.at[i])
        for i, hbm, here in (
            (0, sensor_hbm, modes_out.at[0]),
            (0, source_hbm, modes_out.at[1]),
            (1, source_hbm.at[own], sources.at[my_g, :, 0:modes, :]),
            (1, source_hbm.at[own], sources.at[my_g, :, modes : 2 * modes, :]),
        )
    ]
    for copy in small + owned:
        copy.start()

    raw_copy.wait()
    plus[...] = (raw[0] + raw[1]).reshape(plus.shape)
    my_rows = pl.ds(pl.multiple_of(my_f * row_count, row_count), row_count)
    near_rows = pl.ds(pl.multiple_of(lax.rem(my_f, per) * row_count, row_count), row_count)
    for b in range(nb):
        table[my_g, b, my_rows, :] = plus[my_f, my_g, b]
    if paired:
        away = 1 - home
        away_rows = pl.ds(pl.multiple_of(away * group, group), group)

        @pl.when(straight)
        def _():
            mirror[...] = jnp.zeros_like(mirror)

        @pl.when(crossed)
        def _():
            table[home, :, away_rows, :] = jnp.zeros((nb, group, col_count), jnp.float32)
            minus[...] = (raw[0] - raw[1]).reshape(minus.shape)
            for b in range(nb):
                mirror[b, near_rows, :] = minus[my_f, my_g, b]

    if modes < LANES:
        shapes[:, :, modes:, :] = jnp.zeros((ng, nb, LANES - modes, col_count), jnp.float32)

    settle(modes_out, own_sem.at[0])
    settle(sources.at[my_g], own_sem.at[1])
    for b in range(nb):
        shapes[my_g, b, 0:modes, :] = modes_out[0, my_g * nb + b]
    pl.semaphore_wait(barrier, (plane + 1) * span * ng - 1)
    for k in range(PLANES - 1, 0, -1):

        @pl.when(plane >= k)
        def _():
            signal(known.at[plane], my_f - k * span, my_g)

    def mode_copies(k):
        peer = lax.rem(my_g + k, ng)
        theirs = pl.ds(peer * nb, nb)
        places = (shapes.at[my_g, :, 0:modes, :], sources.at[my_g, :, 0:modes, :])
        return [
            pltpu.make_async_remote_copy(
                src_ref=modes_out.at[i, theirs],
                dst_ref=here,
                send_sem=mode_send.at[k - 1],
                recv_sem=mode_recv.at[k - 1],
                device_id=(my_f, peer),
                device_id_type=MESH,
            )
            for i, here in enumerate(places)
        ]

    def copy_to(source, target, i, f, g):
        return pltpu.make_async_remote_copy(
            src_ref=source,
            dst_ref=target,
            send_sem=send_sem.at[i],
            recv_sem=recv_sem.at[i],
            device_id=(f, g),
            device_id_type=MESH,
        )

    last = away * (nf - span) if paired else 0

    def relay_copy():
        return pltpu.make_async_remote_copy(
            src_ref=plus.at[pl.ds(last, span), 1 - my_g],
            dst_ref=relay,
            send_sem=relay_send,
            recv_sem=relay_recv,
            device_id=(my_f, 1 - my_g),
            device_id_type=MESH,
        )

    def send_near(shift, start):
        peers = [(j, flipped(j)) for j in range(span * ng - 1, start - 1, -1)]
        for j, (f, g) in peers:
            f = f + shift
            copy_to(plus.at[f, g], table.at[my_g, :, my_rows, :], 0, f, g).start()
        if paired:

            @pl.when(crossed)
            def _():
                for j, (f, g) in peers:
                    if j % ng == 0:
                        f = f + shift
                        copy_to(minus.at[f, g], mirror.at[:, near_rows, :], 1, f, g).start()

    def send_far(shift, straight_only, crossed_only):
        ends = (my_f + shift) // span * span == last
        target = table.at[home, :, my_rows, :]

        def sends(source, js):
            for j in js:
                f, g = flipped(j)
                f = f + shift
                copy_to(source(f, g), target, 0, f, g).start()

        if not crossed_only:

            @pl.when(straight & jnp.logical_not(ends))
            def _():
                sends(lambda f, g: plus.at[f, g], range(span * ng - 1, -1, -1))

            @pl.when(straight & ends)
            def _():
                sends(lambda f, g: plus.at[f, g], range((span - 1) * ng, -1, -ng))

        def crossing(direct, forward):
            base = (my_f + shift) // span * span
            for o in sorted(range(span), key=lambda o: (-(o // 2), o)):
                f = base + o
                if direct:
                    copy_to(plus.at[f, my_g], table.at[my_g, :, my_rows, :], 0, f, my_g).start()
                if forward:
                    copy_to(relay.at[f - last], target, 0, f, my_g).start()

        if straight_only:
            pl.when(crossed)(lambda: crossing(True, False))
        elif crossed_only:
            pl.when(crossed & ends)(lambda: crossing(False, True))
        else:
            pl.when(crossed & ends)(lambda: crossing(True, True))
            pl.when(crossed & jnp.logical_not(ends))(lambda: crossing(True, False))

    def send_plane(shift, **which):
        if not paired:
            send_near(shift, 0)
            return
        there = (my_f + shift) // per

        @pl.when(there == home)
        def _():
            send_near(shift, 0)

        @pl.when(there != home)
        def _():
            send_far(shift, **which)

    if paired:

        @pl.when(straight)
        def _():
            relay_copy().start()

    @pl.when(plane > 0)
    def _():
        for k in range(1, ng):
            for copy in mode_copies(k):
                copy.start()

    for copy in small:
        copy.wait()
    radius = 1.0 + lax.broadcasted_iota(jnp.int32, (ranges, LANES), 0).astype(jnp.float32)
    lane = lax.broadcasted_iota(jnp.int32, (ranges, LANES), 1)
    for b in range(nb):
        row = my_g * nb + b
        rows[...] = jnp.ones_like(rows)
        rows[0:1, 0:modes] = wave[pl.ds(row, 1), :]
        rows[1:2, 0:modes] = atten[pl.ds(row, 1), :]
        phase = radius * rows[0:1, :]
        magnitude = jnp.exp(-rows[1:2, :] * radius) / jnp.sqrt(phase)
        magnitude = jnp.where(lane < jnp.minimum(counts[row], modes), magnitude, 0.0)
        first[b, 0] = magnitude * jnp.cos(phase)
        second[b, 0] = magnitude * jnp.sin(phase)

    for b in range(nb):
        real, imag = first[b, 0], second[b, 0]
        ahead = []
        for value in (real + imag, real - imag):
            ahead.append(jnp.where(lane < modes, value, pltpu.roll(value, modes, 1)))
        for d in range(half + 1):
            turned = []
            for value in ahead:
                if d > 0:
                    near = pltpu.roll(value, LANES - d, 1)
                    if modes - 1 + d >= LANES:
                        far = pltpu.roll(value, modes - d, 1)
                        near = jnp.where(lane < LANES - d, near, far)
                    value = near
                turned.append(value)
            total, gap = turned
            one = real * gap + imag * total
            two = real * total - imag * gap
            if d == 0 or 2 * d == modes:
                one, two = 0.5 * one, 0.5 * two
            first[b, d] = one
            second[b, d] = two

    send_near(0, 1)
    for k in range(PLANES - 1, 0, -1):

        @pl.when(plane >= k)
        def _():
            send_plane(-k * span, straight_only=True, crossed_only=False)

    if paired:

        @pl.when(crossed & (plane >= PLANES // 2))
        def _():
            relay_copy().wait_recv()
            for k in range(PLANES // 2, PLANES):

                @pl.when(plane == k)
                def _():
                    send_far(-k * span, False, True)

    for k in range(1, PLANES):

        @pl.when(plane + k < PLANES)
        def _():
            pl.semaphore_wait(known.at[plane + k], 1)
            if paired:

                @pl.when(crossed & (plane < PLANES // 2) & (plane + k == PLANES - 1))
                def _():
                    relay_copy().wait_recv()

            send_plane(k * span, straight_only=False, crossed_only=False)

    @pl.when(plane == 0)
    def _():
        for k in range(1, ng):
            for copy in mode_copies(k):
                copy.start()

    def lay_products(b, g):
        here = sources[g, b, 0:modes, :]
        none = jnp.zeros((LANES - modes, depth_here), jnp.bfloat16)
        for d in range(half + 1):
            pair = here * sources[g, b, d : d + modes, :]
            high, low = split(pair)
            slots = [(0, high), (1, high), (2, low)] if d == 0 else [(d + 2, high)]
            for slot, value in slots:
                right[b, g, slot * LANES : slot * LANES + modes, :] = value
                if modes < LANES:
                    right[b, g, slot * LANES + modes : (slot + 1) * LANES, :] = none

    for k in range(1, ng):
        settle(modes_out.at[:, pl.ds(0, nb)], mode_recv.at[k - 1])

    for b in range(nb):
        for g in range(ng):
            @pl.when(my_g != g)
            def _():
                sources[g, b, modes : 2 * modes, :] = sources[g, b, 0:modes, :]

            lay_products(b, g)

    def slots_of(lefts):
        slots = []
        for d in range(half + 1):
            high, low = split(lefts(d))
            slots += [high, low, high] if d == 0 else [high]
        return slots

    def form(b, g, slots):
        total = None
        for k in range(0, len(slots), CHUNK):
            left = jnp.concatenate(slots[k : k + CHUNK], axis=1)
            end = k + len(slots[k : k + CHUNK])
            part = product(left, right[b, g, k * LANES : end * LANES, :], NN)
            total = part if total is None else total + part
        return total

    def spread(ref, d, count):
        return jnp.broadcast_to(ref[d : d + 1, :], (count, LANES))

    for b in range(nb):
        wide = jnp.concatenate([shapes[g, b] for g in range(ng)], axis=1)
        gram = lax.dot_general(
            wide[0:modes], wide, NT, precision=HIGH, preferred_element_type=jnp.float32
        )
        rows[0:modes, :] = diagonals(gram, modes)
        slots = slots_of(lambda d: spread(rows, d, ranges) * (first[b, d] + second[b, d]))
        for g in range(ng):
            denom[b, g] = form(b, g, slots) * float(devices * nb)

    def pieces(count):
        return raw.at[0, pl.ds(0, count * nb)]

    if paired:

        @pl.when(straight)
        def _():
            settle(pieces(devices - 1), recv_sem.at[0])

        @pl.when(crossed)
        def _():
            settle(pieces(nf + per - 1), recv_sem.at[0])
            settle(pieces(per - 1), recv_sem.at[1])

    else:
        settle(pieces(devices - 1), recv_sem.at[0])

    def part(f, g):
        return pltpu.make_async_remote_copy(
            src_ref=power.at[g, f],
            dst_ref=parts.at[me],
            send_sem=part_send,
            recv_sem=part_recv,
            device_id=(f, g),
            device_id_type=MESH,
        )

    head = max(span * share, 16)
    for b in range(nb):
        blocks = [split(shapes[g, b]) for g in range(ng)]
        left = [jnp.concatenate([block[i] for block in blocks], axis=1) for i in range(2)]

        def projected():
            whole = split(jnp.concatenate([table[g, b] for g in range(ng)], axis=1))
            return thrice(split(thrice(left, whole, modes, NN)), left, modes, NT)

        square = jnp.zeros((LANES - modes, LANES), jnp.float32)

        def turned(value):
            return jnp.concatenate([value, square], 0).T[0:modes]

        def lay(forward, backward):
            rows[0:modes, :] = diagonals(backward, modes)
            rows[LANES : LANES + modes, :] = diagonals(forward, modes)

        if paired:

            @pl.when(straight)
            def _():
                both = projected()
                lay(both, turned(both))

            @pl.when(crossed)
            def _():
                both = projected()
                here, there = split(shapes[home, b]), split(shapes[away, b])
                across = thrice(split(thrice(here, split(mirror[b]), modes, NN)), there, modes, NT)
                lay(both + turned(across), turned(both) + across)

        else:
            both = projected()
            lay(both, turned(both))

        def slots_at(low, high):
            count = high - low
            return slots_of(
                lambda d: spread(rows, d, count) * first[b, d, low:high, :]
                + spread(rows, LANES + d, count) * second[b, d, low:high, :]
            )

        def place(g, low, score):
            score = score / denom[b, g, low : low + score.shape[0], :]
            at = slice(low // share, (low + score.shape[0]) // share)
            value = score.reshape(at.stop - at.start, share, depth_here)
            power[g, at] = value if b == 0 else power[g, at] + value

        early = slots_at(0, head)
        place(0, 0, form(b, 0, early))
        if b == nb - 1:
            for f in range(head // share):

                @pl.when(me != f * ng)
                def _():
                    part(jnp.int32(f), jnp.int32(0)).start()

        late = slots_at(head, ranges)
        if head < ranges:
            place(0, head, form(b, 0, late))
        every = [jnp.concatenate(pair, 0) for pair in zip(early, late)]
        for g in range(1, ng):
            place(g, 0, form(b, g, every))

    for j in range(devices - 1, 0, -1):
        f, g = flipped(j)

        @pl.when((f >= head // share) | (g > 0))
        def _():
            part(f, g).start()

    parts[me] = power[my_g, my_f]

    for k in range(1, ng):
        settle(modes_out.at[:, pl.ds(0, nb)], mode_send.at[k - 1])

    if paired:
        settle(pieces(nf - 1 + nf - span), send_sem.at[0])

        @pl.when(crossed)
        def _():
            settle(pieces(per - 1), send_sem.at[1])

        @pl.when(straight)
        def _():
            relay_copy().wait_send()

    else:
        settle(pieces(devices - 1), send_sem.at[0])

    settle(parts.at[pl.ds(0, devices - 1)], part_send)
    settle(parts.at[pl.ds(0, devices - 1)], part_recv)
    out_ref[...] = jnp.sum(parts[...], axis=0)


def solution(mesh):
    nf, ng = mesh.shape["freq"], mesh.shape["grid"]
    devices = nf * ng

    def per_device(cross_spectra, sensor_modes, source_modes, wavenumber, attenuation, mode_counts):
        two, bins, rows, cols = cross_spectra.shape
        bins_here, modes, _ = sensor_modes.shape
        depth_here = source_modes.shape[2]
        nb = bins_here // ng
        ranges = RANGES // nf * nf
        share = ranges // nf
        slots = modes // 2 + 3
        f32, bf16 = jnp.float32, jnp.bfloat16
        dma = pltpu.SemaphoreType.DMA
        operands = (
            cross_spectra, sensor_modes, source_modes, wavenumber, attenuation, mode_counts
        )
        return pl.pallas_call(
            functools.partial(kernel, nf, ng),
            out_shape=jax.ShapeDtypeStruct((share, depth_here), f32),
            in_specs=[pl.BlockSpec(memory_space=pltpu.HBM)] * 6,
            out_specs=pl.BlockSpec(memory_space=pltpu.VMEM),
            scratch_shapes=[
                pltpu.VMEM((bins_here, modes), f32),
                pltpu.VMEM((bins_here, modes), f32),
                pltpu.SMEM((bins_here,), jnp.int32),
                pltpu.VMEM((two, bins, rows, cols), f32),
                pltpu.VMEM((nf, ng, nb, rows, cols), f32),
                pltpu.VMEM((nf, ng, nb, rows, cols), f32),
                pltpu.VMEM((ng, nb, nf * rows, cols), f32),
                pltpu.VMEM((nb, nf // ng * rows, cols), f32),
                pltpu.VMEM((nf // PLANES, nb, rows, cols), f32),
                pltpu.VMEM((2, bins_here, modes, cols), f32),
                pltpu.VMEM((ng, nb, LANES, cols), f32),
                pltpu.VMEM((ng, nb, 2 * modes, depth_here), f32),
                pltpu.VMEM((nb, modes // 2 + 1, ranges, LANES), f32),
                pltpu.VMEM((nb, modes // 2 + 1, ranges, LANES), f32),
                pltpu.VMEM((nb, ng, slots * LANES, depth_here), bf16),
                pltpu.VMEM((2 * LANES, LANES), f32),
                pltpu.VMEM((nb, ng, ranges, depth_here), f32),
                pltpu.VMEM((ng, nf, share, depth_here), f32),
                pltpu.VMEM((devices, share, depth_here), f32),
                pltpu.SemaphoreType.REGULAR((PLANES,)),
                dma((3,)), dma, dma((2,)), dma((max(ng - 1, 1),)), dma((max(ng - 1, 1),)),
                dma((2,)), dma((2,)), dma, dma, dma, dma,
            ],
            compiler_params=pltpu.CompilerParams(
                collective_id=0, has_side_effects=True, vmem_limit_bytes=32 * 1024 * 1024
            ),
        )(*[pltpu.with_memory_space_constraint(x, pltpu.HBM) for x in operands])

    placed = (
        P(None, None, "freq", "grid"),
        P("freq", None, "grid"),
        P("freq", None, "grid"),
        P("freq", None),
        P("freq", None),
        P("freq"),
    )
    return jax.shard_map(
        per_device, mesh=mesh, in_specs=placed, out_specs=P("freq", "grid"), check_vma=False
    )
```

```python
import functools

import jax
import jax.numpy as jnp
from jax import lax
from jax.experimental import pallas as pl
from jax.experimental.pallas import tpu as pltpu
from jax.sharding import PartitionSpec as P

RANGES = 64
LANES = 128
CHUNK = 2
PLANES = 4

HIGH = lax.Precision.HIGHEST
MESH = pl.DeviceIdType.MESH
NT = (((1,), (1,)), ((), ()))
NN = (((1,), (0,)), ((), ()))


def split(value):
    high = value.astype(jnp.bfloat16)
    return high, (value - high.astype(jnp.float32)).astype(jnp.bfloat16)


def product(left, right, dims):
    return lax.dot_general(left, right, dims, preferred_element_type=jnp.float32)


def thrice(left, right, rows, dims):
    high, low = left[0][0:rows], left[1][0:rows]
    both = product(jnp.concatenate([high, low], 0), right[0], dims)
    return both[:rows] + (both[rows:] + product(high, right[1], dims))


def diagonals(square, modes):
    lane = lax.broadcasted_iota(jnp.int32, square.shape, 1)
    step = 1
    while step < modes:
        turned = pltpu.roll(square, modes - step, 0)
        square = jnp.where(lax.rem(lane // step, 2) == 1, turned, square)
        step *= 2
    return square


def kernel(
    nf, ng,
    spectra_hbm, sensor_hbm, source_hbm, wave_hbm, atten_hbm, counts_hbm,
    out_ref,
    wave, atten, counts, raw, plus, minus, table, mirror, relay, modes_out, shapes, sources,
    first, second, right, rows, denom, power, parts,
    known, small_sem, raw_sem, own_sem, mode_send, mode_recv, send_sem, recv_sem,
    relay_send, relay_recv, part_send, part_recv,
):
    devices = nf * ng
    nb, row_count, col_count = plus.shape[2:]
    paired = ng == 2
    per = nf // ng
    group = per * row_count
    modes = modes_out.shape[2]
    half = modes // 2
    ranges = first.shape[2]
    share = ranges // nf
    depth_here = sources.shape[3]
    my_f, my_g = lax.axis_index("freq"), lax.axis_index("grid")
    me = my_f * ng + my_g
    home = my_f // per
    crossed = home != my_g
    straight = home == my_g

    barrier = pltpu.get_barrier_semaphore()
    span = nf // PLANES
    plane = my_f // span

    def flips(index, size):
        deltas, weight = [], 1
        while weight < size:
            deltas.append((1 - 2 * lax.rem(index // weight, 2)) * weight)
            weight *= 2
        return deltas

    flip_f, flip_g = flips(my_f, nf), flips(my_g, ng)

    def flipped(j):
        f, g = my_f, my_g
        for bit, delta in enumerate(flip_g + flip_f):
            if j >> bit & 1:
                if bit < len(flip_g):
                    g = g + delta
                else:
                    f = f + delta
        return f, g

    def signal(semaphore, f, g):
        pl.semaphore_signal(semaphore, inc=1, device_id=(f, g), device_id_type=MESH)

    def greet(f, carry):
        for g in range(ng):
            signal(barrier, nf + (plane + 1) * span - 1 - f, g)
        return carry

    lax.fori_loop((plane + 1) * span, nf, greet, 0)
    for j in range(span * ng - 1, 0, -1):
        signal(barrier, *flipped(j))

    def settle(ref, sem):
        pltpu.make_async_copy(ref, ref, sem).wait()

    raw_copy = pltpu.make_async_copy(spectra_hbm, raw, raw_sem)
    raw_copy.start()
    small = [
        pltpu.make_async_copy(hbm, here, small_sem.at[i])
        for i, (hbm, here) in enumerate(((wave_hbm, wave), (atten_hbm, atten), (counts_hbm, counts)))
    ]
    own = pl.ds(my_g * nb, nb)
    owned = [
        pltpu.make_async_copy(hbm, here, own_sem.at[i])
        for i, hbm, here in (
            (0, sensor_hbm, modes_out.at[0]),
            (0, source_hbm, modes_out.at[1]),
            (1, source_hbm.at[own], sources.at[my_g, :, 0:modes, :]),
            (1, source_hbm.at[own], sources.at[my_g, :, modes : 2 * modes, :]),
        )
    ]
    for copy in small + owned:
        copy.start()

    raw_copy.wait()
    plus[...] = (raw[0] + raw[1]).reshape(plus.shape)
    my_rows = pl.ds(pl.multiple_of(my_f * row_count, row_count), row_count)
    near_rows = pl.ds(pl.multiple_of(lax.rem(my_f, per) * row_count, row_count), row_count)
    for b in range(nb):
        table[my_g, b, my_rows, :] = plus[my_f, my_g, b]
    if paired:
        away = 1 - home
        away_rows = pl.ds(pl.multiple_of(away * group, group), group)

        @pl.when(straight)
        def _():
            mirror[...] = jnp.zeros_like(mirror)

        @pl.when(crossed)
        def _():
            table[home, :, away_rows, :] = jnp.zeros((nb, group, col_count), jnp.float32)
            minus[...] = (raw[0] - raw[1]).reshape(minus.shape)
            for b in range(nb):
                mirror[b, near_rows, :] = minus[my_f, my_g, b]

    if modes < LANES:
        shapes[:, :, modes:, :] = jnp.zeros((ng, nb, LANES - modes, col_count), jnp.float32)

    settle(modes_out, own_sem.at[0])
    settle(sources.at[my_g], own_sem.at[1])
    for b in range(nb):
        shapes[my_g, b, 0:modes, :] = modes_out[0, my_g * nb + b]
    pl.semaphore_wait(barrier, (plane + 1) * span * ng - 1)
    for k in range(PLANES - 1, 0, -1):

        @pl.when(plane >= k)
        def _():
            signal(known.at[plane], my_f - k * span, my_g)

    def mode_copies(k):
        peer = lax.rem(my_g + k, ng)
        theirs = pl.ds(peer * nb, nb)
        places = (shapes.at[my_g, :, 0:modes, :], sources.at[my_g, :, 0:modes, :])
        return [
            pltpu.make_async_remote_copy(
                src_ref=modes_out.at[i, theirs],
                dst_ref=here,
                send_sem=mode_send.at[k - 1],
                recv_sem=mode_recv.at[k - 1],
                device_id=(my_f, peer),
                device_id_type=MESH,
            )
            for i, here in enumerate(places)
        ]

    def copy_to(source, target, i, f, g):
        return pltpu.make_async_remote_copy(
            src_ref=source,
            dst_ref=target,
            send_sem=send_sem.at[i],
            recv_sem=recv_sem.at[i],
            device_id=(f, g),
            device_id_type=MESH,
        )

    last = away * (nf - span) if paired else 0

    def relay_copy():
        return pltpu.make_async_remote_copy(
            src_ref=plus.at[pl.ds(last, span), 1 - my_g],
            dst_ref=relay,
            send_sem=relay_send,
            recv_sem=relay_recv,
            device_id=(my_f, 1 - my_g),
            device_id_type=MESH,
        )

    def send_near(shift, start):
        peers = [(j, flipped(j)) for j in range(span * ng - 1, start - 1, -1)]
        for j, (f, g) in peers:
            f = f + shift
            copy_to(plus.at[f, g], table.at[my_g, :, my_rows, :], 0, f, g).start()
        if paired:

            @pl.when(crossed)
            def _():
                for j, (f, g) in peers:
                    if j % ng == 0:
                        f = f + shift
                        copy_to(minus.at[f, g], mirror.at[:, near_rows, :], 1, f, g).start()

    def send_far(shift, straight_only, crossed_only):
        ends = (my_f + shift) // span * span == last
        target = table.at[home, :, my_rows, :]

        base = (my_f + shift) // span * span
        order = sorted(range(span), key=lambda o: (-(o // 2), o))

        def sends(grids):
            for o in order:
                for g in grids:
                    f = base + o
                    copy_to(plus.at[f, g], target, 0, f, g).start()

        if not crossed_only:
            pl.when(straight & jnp.logical_not(ends))(lambda: sends((1 - my_g, my_g)))
            pl.when(straight & ends)(lambda: sends((my_g,)))

        def crossing(direct, forward):
            for o in order:
                f = base + o
                if direct:
                    copy_to(plus.at[f, my_g], table.at[my_g, :, my_rows, :], 0, f, my_g).start()
                if forward:
                    copy_to(relay.at[f - last], target, 0, f, my_g).start()

        if straight_only:
            pl.when(crossed)(lambda: crossing(True, False))
        elif crossed_only:
            pl.when(crossed & ends)(lambda: crossing(False, True))
        else:
            pl.when(crossed & ends)(lambda: crossing(True, True))
            pl.when(crossed & jnp.logical_not(ends))(lambda: crossing(True, False))

    def send_plane(shift, **which):
        if not paired:
            send_near(shift, 0)
            return
        there = (my_f + shift) // per

        @pl.when(there == home)
        def _():
            send_near(shift, 0)

        @pl.when(there != home)
        def _():
            send_far(shift, **which)

    if paired:

        @pl.when(straight)
        def _():
            relay_copy().start()

    @pl.when(plane > 0)
    def _():
        for k in range(1, ng):
            for copy in mode_copies(k):
                copy.start()

    @pl.when(plane == PLANES - 1)
    def _():
        send_near(0, 1)
        for k in range(PLANES - 1, 0, -1):

            @pl.when(plane >= k)
            def _():
                send_plane(-k * span, straight_only=True, crossed_only=False)

    for copy in small:
        copy.wait()
    radius = 1.0 + lax.broadcasted_iota(jnp.int32, (ranges, LANES), 0).astype(jnp.float32)
    lane = lax.broadcasted_iota(jnp.int32, (ranges, LANES), 1)
    for b in range(nb):
        row = my_g * nb + b
        rows[...] = jnp.ones_like(rows)
        rows[0:1, 0:modes] = wave[pl.ds(row, 1), :]
        rows[1:2, 0:modes] = atten[pl.ds(row, 1), :]
        phase = radius * rows[0:1, :]
        magnitude = jnp.exp(-rows[1:2, :] * radius) / jnp.sqrt(phase)
        magnitude = jnp.where(lane < jnp.minimum(counts[row], modes), magnitude, 0.0)
        first[b, 0] = magnitude * jnp.cos(phase)
        second[b, 0] = magnitude * jnp.sin(phase)

    for b in range(nb):
        real, imag = first[b, 0], second[b, 0]
        ahead = []
        for value in (real + imag, real - imag):
            ahead.append(jnp.where(lane < modes, value, pltpu.roll(value, modes, 1)))
        for d in range(half + 1):
            turned = []
            for value in ahead:
                if d > 0:
                    near = pltpu.roll(value, LANES - d, 1)
                    if modes - 1 + d >= LANES:
                        far = pltpu.roll(value, modes - d, 1)
                        near = jnp.where(lane < LANES - d, near, far)
                    value = near
                turned.append(value)
            total, gap = turned
            one = real * gap + imag * total
            two = real * total - imag * gap
            if d == 0 or 2 * d == modes:
                one, two = 0.5 * one, 0.5 * two
            first[b, d] = one
            second[b, d] = two

    @pl.when(plane < PLANES - 1)
    def _():
        send_near(0, 1)
        for k in range(PLANES - 1, 0, -1):

            @pl.when(plane >= k)
            def _():
                send_plane(-k * span, straight_only=True, crossed_only=False)

    if paired:

        @pl.when(crossed & (plane >= PLANES // 2))
        def _():
            relay_copy().wait_recv()
            for k in range(PLANES // 2, PLANES):

                @pl.when(plane == k)
                def _():
                    send_far(-k * span, False, True)

    for k in range(1, PLANES):

        @pl.when(plane + k < PLANES)
        def _():
            pl.semaphore_wait(known.at[plane + k], 1)
            if paired:

                @pl.when(crossed & (plane < PLANES // 2) & (plane + k == PLANES - 1))
                def _():
                    relay_copy().wait_recv()

            send_plane(k * span, straight_only=False, crossed_only=False)

    @pl.when(plane == 0)
    def _():
        for k in range(1, ng):
            for copy in mode_copies(k):
                copy.start()

    def lay_products(b, g):
        here = sources[g, b, 0:modes, :]
        none = jnp.zeros((LANES - modes, depth_here), jnp.bfloat16)
        for d in range(half + 1):
            pair = here * sources[g, b, d : d + modes, :]
            high, low = split(pair)
            slots = [(0, high), (1, high), (2, low)] if d == 0 else [(d + 2, high)]
            for slot, value in slots:
                right[b, g, slot * LANES : slot * LANES + modes, :] = value
                if modes < LANES:
                    right[b, g, slot * LANES + modes : (slot + 1) * LANES, :] = none

    for k in range(1, ng):
        settle(modes_out.at[:, pl.ds(0, nb)], mode_recv.at[k - 1])

    for b in range(nb):
        for g in range(ng):
            @pl.when(my_g != g)
            def _():
                sources[g, b, modes : 2 * modes, :] = sources[g, b, 0:modes, :]

            lay_products(b, g)

    def slots_of(lefts):
        slots = []
        for d in range(half + 1):
            high, low = split(lefts(d))
            slots += [high, low, high] if d == 0 else [high]
        return slots

    def form(b, g, slots):
        total = None
        for k in range(0, len(slots), CHUNK):
            left = jnp.concatenate(slots[k : k + CHUNK], axis=1)
            end = k + len(slots[k : k + CHUNK])
            part = product(left, right[b, g, k * LANES : end * LANES, :], NN)
            total = part if total is None else total + part
        return total

    def spread(ref, d, count):
        return jnp.broadcast_to(ref[d : d + 1, :], (count, LANES))

    for b in range(nb):
        wide = jnp.concatenate([shapes[g, b] for g in range(ng)], axis=1)
        gram = lax.dot_general(
            wide[0:modes], wide, NT, precision=HIGH, preferred_element_type=jnp.float32
        )
        rows[0:modes, :] = diagonals(gram, modes)
        slots = slots_of(lambda d: spread(rows, d, ranges) * (first[b, d] + second[b, d]))
        for g in range(ng):
            denom[b, g] = form(b, g, slots) * float(devices * nb)

    def pieces(count):
        return raw.at[0, pl.ds(0, count * nb)]

    if paired:

        @pl.when(straight)
        def _():
            settle(pieces(devices - 1), recv_sem.at[0])

        @pl.when(crossed)
        def _():
            settle(pieces(nf + per - 1), recv_sem.at[0])
            settle(pieces(per - 1), recv_sem.at[1])

    else:
        settle(pieces(devices - 1), recv_sem.at[0])

    def part(f, g):
        return pltpu.make_async_remote_copy(
            src_ref=power.at[g, f],
            dst_ref=parts.at[me],
            send_sem=part_send,
            recv_sem=part_recv,
            device_id=(f, g),
            device_id_type=MESH,
        )

    head = max(span * share, 16)
    for b in range(nb):
        blocks = [split(shapes[g, b]) for g in range(ng)]
        left = [jnp.concatenate([block[i] for block in blocks], axis=1) for i in range(2)]

        def projected():
            whole = split(jnp.concatenate([table[g, b] for g in range(ng)], axis=1))
            return thrice(split(thrice(left, whole, modes, NN)), left, modes, NT)

        square = jnp.zeros((LANES - modes, LANES), jnp.float32)

        def turned(value):
            return jnp.concatenate([value, square], 0).T[0:modes]

        def lay(forward, backward):
            rows[0:modes, :] = diagonals(backward, modes)
            rows[LANES : LANES + modes, :] = diagonals(forward, modes)

        if paired:

            @pl.when(straight)
            def _():
                both = projected()
                lay(both, turned(both))

            @pl.when(crossed)
            def _():
                both = projected()
                here, there = split(shapes[home, b]), split(shapes[away, b])
                across = thrice(split(thrice(here, split(mirror[b]), modes, NN)), there, modes, NT)
                lay(both + turned(across), turned(both) + across)

        else:
            both = projected()
            lay(both, turned(both))

        def slots_at(low, high):
            count = high - low
            return slots_of(
                lambda d: spread(rows, d, count) * first[b, d, low:high, :]
                + spread(rows, LANES + d, count) * second[b, d, low:high, :]
            )

        def place(g, low, score):
            score = score / denom[b, g, low : low + score.shape[0], :]
            at = slice(low // share, (low + score.shape[0]) // share)
            value = score.reshape(at.stop - at.start, share, depth_here)
            power[g, at] = value if b == 0 else power[g, at] + value

        early = slots_at(0, head)
        place(0, 0, form(b, 0, early))
        if b == nb - 1:
            for f in range(head // share):

                @pl.when(me != f * ng)
                def _():
                    part(jnp.int32(f), jnp.int32(0)).start()

        late = slots_at(head, ranges)
        if head < ranges:
            place(0, head, form(b, 0, late))
        every = [jnp.concatenate(pair, 0) for pair in zip(early, late)]
        for g in range(1, ng):
            place(g, 0, form(b, g, every))

    for j in range(devices - 1, 0, -1):
        f, g = flipped(j)

        @pl.when((f >= head // share) | (g > 0))
        def _():
            part(f, g).start()

    parts[me] = power[my_g, my_f]

    for k in range(1, ng):
        settle(modes_out.at[:, pl.ds(0, nb)], mode_send.at[k - 1])

    if paired:
        settle(pieces(nf - 1 + nf - span), send_sem.at[0])

        @pl.when(crossed)
        def _():
            settle(pieces(per - 1), send_sem.at[1])

        @pl.when(straight)
        def _():
            relay_copy().wait_send()

    else:
        settle(pieces(devices - 1), send_sem.at[0])

    settle(parts.at[pl.ds(0, devices - 1)], part_send)
    settle(parts.at[pl.ds(0, devices - 1)], part_recv)
    out_ref[...] = jnp.sum(parts[...], axis=0)


def solution(mesh):
    nf, ng = mesh.shape["freq"], mesh.shape["grid"]
    devices = nf * ng

    def per_device(cross_spectra, sensor_modes, source_modes, wavenumber, attenuation, mode_counts):
        two, bins, rows, cols = cross_spectra.shape
        bins_here, modes, _ = sensor_modes.shape
        depth_here = source_modes.shape[2]
        nb = bins_here // ng
        ranges = RANGES // nf * nf
        share = ranges // nf
        slots = modes // 2 + 3
        f32, bf16 = jnp.float32, jnp.bfloat16
        dma = pltpu.SemaphoreType.DMA
        operands = (
            cross_spectra, sensor_modes, source_modes, wavenumber, attenuation, mode_counts
        )
        return pl.pallas_call(
            functools.partial(kernel, nf, ng),
            out_shape=jax.ShapeDtypeStruct((share, depth_here), f32),
            in_specs=[pl.BlockSpec(memory_space=pltpu.HBM)] * 6,
            out_specs=pl.BlockSpec(memory_space=pltpu.VMEM),
            scratch_shapes=[
                pltpu.VMEM((bins_here, modes), f32),
                pltpu.VMEM((bins_here, modes), f32),
                pltpu.SMEM((bins_here,), jnp.int32),
                pltpu.VMEM((two, bins, rows, cols), f32),
                pltpu.VMEM((nf, ng, nb, rows, cols), f32),
                pltpu.VMEM((nf, ng, nb, rows, cols), f32),
                pltpu.VMEM((ng, nb, nf * rows, cols), f32),
                pltpu.VMEM((nb, nf // ng * rows, cols), f32),
                pltpu.VMEM((nf // PLANES, nb, rows, cols), f32),
                pltpu.VMEM((2, bins_here, modes, cols), f32),
                pltpu.VMEM((ng, nb, LANES, cols), f32),
                pltpu.VMEM((ng, nb, 2 * modes, depth_here), f32),
                pltpu.VMEM((nb, modes // 2 + 1, ranges, LANES), f32),
                pltpu.VMEM((nb, modes // 2 + 1, ranges, LANES), f32),
                pltpu.VMEM((nb, ng, slots * LANES, depth_here), bf16),
                pltpu.VMEM((2 * LANES, LANES), f32),
                pltpu.VMEM((nb, ng, ranges, depth_here), f32),
                pltpu.VMEM((ng, nf, share, depth_here), f32),
                pltpu.VMEM((devices, share, depth_here), f32),
                pltpu.SemaphoreType.REGULAR((PLANES,)),
                dma((3,)), dma, dma((2,)), dma((max(ng - 1, 1),)), dma((max(ng - 1, 1),)),
                dma((2,)), dma((2,)), dma, dma, dma, dma,
            ],
            compiler_params=pltpu.CompilerParams(
                collective_id=0, has_side_effects=True, vmem_limit_bytes=32 * 1024 * 1024
            ),
        )(*[pltpu.with_memory_space_constraint(x, pltpu.HBM) for x in operands])

    placed = (
        P(None, None, "freq", "grid"),
        P("freq", None, "grid"),
        P("freq", None, "grid"),
        P("freq", None),
        P("freq", None),
        P("freq"),
    )
    return jax.shard_map(
        per_device, mesh=mesh, in_specs=placed, out_specs=P("freq", "grid"), check_vma=False
    )
```

```python
import functools

import jax
import jax.numpy as jnp
from jax import lax
from jax.experimental import pallas as pl
from jax.experimental.pallas import tpu as pltpu
from jax.sharding import PartitionSpec as P

RANGES = 64
LANES = 128
CHUNK = 2
PLANES = 4

HIGH = lax.Precision.HIGHEST
MESH = pl.DeviceIdType.MESH
NT = (((1,), (1,)), ((), ()))
NN = (((1,), (0,)), ((), ()))


def split(value):
    high = value.astype(jnp.bfloat16)
    return high, (value - high.astype(jnp.float32)).astype(jnp.bfloat16)


def product(left, right, dims):
    return lax.dot_general(left, right, dims, preferred_element_type=jnp.float32)


def thrice(left, right, rows, dims):
    high, low = left[0][0:rows], left[1][0:rows]
    both = product(jnp.concatenate([high, low], 0), right[0], dims)
    return both[:rows] + (both[rows:] + product(high, right[1], dims))


def diagonals(square, modes):
    lane = lax.broadcasted_iota(jnp.int32, square.shape, 1)
    step = 1
    while step < modes:
        turned = pltpu.roll(square, modes - step, 0)
        square = jnp.where(lax.rem(lane // step, 2) == 1, turned, square)
        step *= 2
    return square


def kernel(
    nf, ng,
    spectra_hbm, sensor_hbm, source_hbm, wave_hbm, atten_hbm, counts_hbm,
    out_ref,
    tables, counts, raw, plus, minus, table, mirror, relay, modes_out, shapes, sources,
    first, second, right, rows, denom, power, parts,
    known, small_sem, raw_sem, own_sem, mode_send, mode_recv, send_sem, recv_sem,
    relay_send, relay_recv, part_send, part_recv,
):
    devices = nf * ng
    nb, row_count, col_count = plus.shape[2:]
    paired = ng == 2
    per = nf // ng
    group = per * row_count
    modes = modes_out.shape[2]
    half = modes // 2
    ranges = first.shape[2]
    share = ranges // nf
    depth_here = sources.shape[3]
    my_f, my_g = lax.axis_index("freq"), lax.axis_index("grid")
    me = my_f * ng + my_g
    home = my_f // per
    crossed = home != my_g
    straight = home == my_g

    barrier = pltpu.get_barrier_semaphore()
    span = nf // PLANES
    plane = my_f // span

    def flips(index, size):
        deltas, weight = [], 1
        while weight < size:
            deltas.append((1 - 2 * lax.rem(index // weight, 2)) * weight)
            weight *= 2
        return deltas

    flip_f, flip_g = flips(my_f, nf), flips(my_g, ng)

    def flipped(j):
        f, g = my_f, my_g
        for bit, delta in enumerate(flip_g + flip_f):
            if j >> bit & 1:
                if bit < len(flip_g):
                    g = g + delta
                else:
                    f = f + delta
        return f, g

    def signal(semaphore, f, g):
        pl.semaphore_signal(semaphore, inc=1, device_id=(f, g), device_id_type=MESH)

    def greet(f, carry):
        for g in range(ng):
            signal(barrier, nf + (plane + 1) * span - 1 - f, g)
        return carry

    lax.fori_loop((plane + 1) * span, nf, greet, 0)
    for j in range(span * ng - 1, 0, -1):
        signal(barrier, *flipped(j))

    def settle(ref, sem):
        pltpu.make_async_copy(ref, ref, sem).wait()

    raw_copy = pltpu.make_async_copy(spectra_hbm, raw, raw_sem)
    raw_copy.start()
    small = [
        pltpu.make_async_copy(hbm, here, small_sem.at[i])
        for i, hbm, here in (((0, wave_hbm, tables.at[0]), (0, atten_hbm, tables.at[1]), (1, counts_hbm, counts)))
    ]
    own = pl.ds(my_g * nb, nb)
    owned = [
        pltpu.make_async_copy(hbm, here, own_sem.at[i])
        for i, hbm, here in (
            (0, sensor_hbm, modes_out.at[0]),
            (0, source_hbm, modes_out.at[1]),
            (1, source_hbm.at[own], sources.at[my_g, :, 0:modes, :]),
            (1, source_hbm.at[own], sources.at[my_g, :, modes : 2 * modes, :]),
        )
    ]
    for copy in small + owned:
        copy.start()

    raw_copy.wait()
    plus[...] = (raw[0] + raw[1]).reshape(plus.shape)
    my_rows = pl.ds(pl.multiple_of(my_f * row_count, row_count), row_count)
    near_rows = pl.ds(pl.multiple_of(lax.rem(my_f, per) * row_count, row_count), row_count)
    for b in range(nb):
        table[my_g, b, my_rows, :] = plus[my_f, my_g, b]
    if paired:
        away = 1 - home
        away_rows = pl.ds(pl.multiple_of(away * group, group), group)

        @pl.when(straight)
        def _():
            mirror[...] = jnp.zeros_like(mirror)

        @pl.when(crossed)
        def _():
            table[home, :, away_rows, :] = jnp.zeros((nb, group, col_count), jnp.float32)
            minus[...] = (raw[0] - raw[1]).reshape(minus.shape)
            for b in range(nb):
                mirror[b, near_rows, :] = minus[my_f, my_g, b]

    if modes < LANES:
        shapes[:, :, modes:, :] = jnp.zeros((ng, nb, LANES - modes, col_count), jnp.float32)

    settle(modes_out, own_sem.at[0])
    settle(sources.at[my_g], own_sem.at[1])
    for b in range(nb):
        shapes[my_g, b, 0:modes, :] = modes_out[0, my_g * nb + b]
    pl.semaphore_wait(barrier, (plane + 1) * span * ng - 1)
    for k in range(PLANES - 1, 0, -1):

        @pl.when(plane >= k)
        def _():
            signal(known.at[plane - 1], my_f - k * span, my_g)

    def mode_copies(k):
        peer = lax.rem(my_g + k, ng)
        theirs = pl.ds(peer * nb, nb)
        places = (shapes.at[my_g, :, 0:modes, :], sources.at[my_g, :, 0:modes, :])
        return [
            pltpu.make_async_remote_copy(
                src_ref=modes_out.at[i, theirs],
                dst_ref=here,
                send_sem=mode_send.at[k - 1],
                recv_sem=mode_recv.at[k - 1],
                device_id=(my_f, peer),
                device_id_type=MESH,
            )
            for i, here in enumerate(places)
        ]

    def copy_to(source, target, i, f, g):
        return pltpu.make_async_remote_copy(
            src_ref=source,
            dst_ref=target,
            send_sem=send_sem.at[i],
            recv_sem=recv_sem.at[i],
            device_id=(f, g),
            device_id_type=MESH,
        )

    last = away * (nf - span) if paired else 0

    def relay_copy():
        return pltpu.make_async_remote_copy(
            src_ref=plus.at[pl.ds(last, span), 1 - my_g],
            dst_ref=relay,
            send_sem=relay_send,
            recv_sem=relay_recv,
            device_id=(my_f, 1 - my_g),
            device_id_type=MESH,
        )

    def send_near(shift, start):
        peers = [(j, flipped(j)) for j in range(span * ng - 1, start - 1, -1)]
        for j, (f, g) in peers:
            f = f + shift
            copy_to(plus.at[f, g], table.at[my_g, :, my_rows, :], 0, f, g).start()
        if paired:

            @pl.when(crossed)
            def _():
                for j, (f, g) in peers:
                    if j % ng == 0:
                        f = f + shift
                        copy_to(minus.at[f, g], mirror.at[:, near_rows, :], 1, f, g).start()

    def send_far(shift, straight_only, crossed_only):
        ends = (my_f + shift) // span * span == last
        target = table.at[home, :, my_rows, :]

        base = (my_f + shift) // span * span
        order = sorted(range(span), key=lambda o: (-(o // 2), o))

        def sends(grids):
            for o in order:
                for g in grids:
                    f = base + o
                    copy_to(plus.at[f, g], target, 0, f, g).start()

        if not crossed_only:
            pl.when(straight & jnp.logical_not(ends))(lambda: sends((1 - my_g, my_g)))
            pl.when(straight & ends)(lambda: sends((my_g,)))

        def crossing(direct, forward):
            for o in order:
                f = base + o
                if direct:
                    copy_to(plus.at[f, my_g], table.at[my_g, :, my_rows, :], 0, f, my_g).start()
                if forward:
                    copy_to(relay.at[f - last], target, 0, f, my_g).start()

        if straight_only:
            pl.when(crossed)(lambda: crossing(True, False))
        elif crossed_only:
            pl.when(crossed & ends)(lambda: crossing(False, True))
        else:
            pl.when(crossed & ends)(lambda: crossing(True, True))
            pl.when(crossed & jnp.logical_not(ends))(lambda: crossing(True, False))

    def send_plane(shift, **which):
        if not paired:
            send_near(shift, 0)
            return
        there = (my_f + shift) // per

        @pl.when(there == home)
        def _():
            send_near(shift, 0)

        @pl.when(there != home)
        def _():
            send_far(shift, **which)

    if paired:

        @pl.when(straight)
        def _():
            relay_copy().start()

    @pl.when(plane > 0)
    def _():
        for k in range(1, ng):
            for copy in mode_copies(k):
                copy.start()

    @pl.when(plane == PLANES - 1)
    def _():
        send_near(0, 1)
        for k in range(PLANES - 1, 0, -1):

            @pl.when(plane >= k)
            def _():
                send_plane(-k * span, straight_only=True, crossed_only=False)

    settle(tables, small_sem.at[0])
    small[2].wait()
    radius = 1.0 + lax.broadcasted_iota(jnp.int32, (ranges, LANES), 0).astype(jnp.float32)
    lane = lax.broadcasted_iota(jnp.int32, (ranges, LANES), 1)
    for b in range(nb):
        row = my_g * nb + b
        rows[...] = jnp.ones_like(rows)
        rows[0:1, 0:modes] = tables[0, pl.ds(row, 1), :]
        rows[1:2, 0:modes] = tables[1, pl.ds(row, 1), :]
        phase = radius * rows[0:1, :]
        magnitude = jnp.exp(-rows[1:2, :] * radius) / jnp.sqrt(phase)
        magnitude = jnp.where(lane < jnp.minimum(counts[row], modes), magnitude, 0.0)
        first[b, 0] = magnitude * jnp.cos(phase)
        second[b, 0] = magnitude * jnp.sin(phase)

    for b in range(nb):
        real, imag = first[b, 0], second[b, 0]
        ahead = []
        for value in (real + imag, real - imag):
            ahead.append(jnp.where(lane < modes, value, pltpu.roll(value, modes, 1)))
        for d in range(half + 1):
            turned = []
            for value in ahead:
                if d > 0:
                    near = pltpu.roll(value, LANES - d, 1)
                    if modes - 1 + d >= LANES:
                        far = pltpu.roll(value, modes - d, 1)
                        near = jnp.where(lane < LANES - d, near, far)
                    value = near
                turned.append(value)
            total, gap = turned
            one = real * gap + imag * total
            two = real * total - imag * gap
            if d == 0 or 2 * d == modes:
                one, two = 0.5 * one, 0.5 * two
            first[b, d] = one
            second[b, d] = two

    @pl.when(plane < PLANES - 1)
    def _():
        send_near(0, 1)
        for k in range(PLANES - 1, 0, -1):

            @pl.when(plane >= k)
            def _():
                send_plane(-k * span, straight_only=True, crossed_only=False)

    if paired:

        @pl.when(crossed & (plane >= PLANES // 2))
        def _():
            relay_copy().wait_recv()
            for k in range(PLANES // 2, PLANES):

                @pl.when(plane == k)
                def _():
                    send_far(-k * span, False, True)

    for k in range(1, PLANES):

        @pl.when(plane + k < PLANES)
        def _():
            pl.semaphore_wait(known.at[plane + k - 1], 1)
            if paired:

                @pl.when(crossed & (plane < PLANES // 2) & (plane + k == PLANES - 1))
                def _():
                    relay_copy().wait_recv()

            send_plane(k * span, straight_only=False, crossed_only=False)

    @pl.when(plane == 0)
    def _():
        for k in range(1, ng):
            for copy in mode_copies(k):
                copy.start()

    def lay_products(b, g):
        here = sources[g, b, 0:modes, :]
        none = jnp.zeros((LANES - modes, depth_here), jnp.bfloat16)
        for d in range(half + 1):
            pair = here * sources[g, b, d : d + modes, :]
            high, low = split(pair)
            slots = [(0, high), (1, high), (2, low)] if d == 0 else [(d + 2, high)]
            for slot, value in slots:
                right[b, g, slot * LANES : slot * LANES + modes, :] = value
                if modes < LANES:
                    right[b, g, slot * LANES + modes : (slot + 1) * LANES, :] = none

    for k in range(1, ng):
        settle(modes_out.at[:, pl.ds(0, nb)], mode_recv.at[k - 1])

    for b in range(nb):
        for g in range(ng):
            @pl.when(my_g != g)
            def _():
                sources[g, b, modes : 2 * modes, :] = sources[g, b, 0:modes, :]

            lay_products(b, g)

    def slots_of(lefts):
        slots = []
        for d in range(half + 1):
            high, low = split(lefts(d))
            slots += [high, low, high] if d == 0 else [high]
        return slots

    def form(b, g, slots):
        total = None
        for k in range(0, len(slots), CHUNK):
            left = jnp.concatenate(slots[k : k + CHUNK], axis=1)
            end = k + len(slots[k : k + CHUNK])
            part = product(left, right[b, g, k * LANES : end * LANES, :], NN)
            total = part if total is None else total + part
        return total

    def spread(ref, d, count):
        return jnp.broadcast_to(ref[d : d + 1, :], (count, LANES))

    for b in range(nb):
        wide = jnp.concatenate([shapes[g, b] for g in range(ng)], axis=1)
        gram = lax.dot_general(
            wide[0:modes], wide, NT, precision=HIGH, preferred_element_type=jnp.float32
        )
        rows[0:modes, :] = diagonals(gram, modes)
        slots = slots_of(lambda d: spread(rows, d, ranges) * (first[b, d] + second[b, d]))
        for g in range(ng):
            denom[b, g] = form(b, g, slots) * float(devices * nb)

    def pieces(count):
        return raw.at[0, pl.ds(0, count * nb)]

    if paired:

        @pl.when(straight)
        def _():
            settle(pieces(devices - 1), recv_sem.at[0])

        @pl.when(crossed)
        def _():
            settle(pieces(nf + per - 1), recv_sem.at[0])
            settle(pieces(per - 1), recv_sem.at[1])

    else:
        settle(pieces(devices - 1), recv_sem.at[0])

    def part(f, g):
        return pltpu.make_async_remote_copy(
            src_ref=power.at[g, f],
            dst_ref=parts.at[me],
            send_sem=part_send,
            recv_sem=part_recv,
            device_id=(f, g),
            device_id_type=MESH,
        )

    head = max(span * share, 16)
    for b in range(nb):
        blocks = [split(shapes[g, b]) for g in range(ng)]
        left = [jnp.concatenate([block[i] for block in blocks], axis=1) for i in range(2)]

        def projected():
            whole = split(jnp.concatenate([table[g, b] for g in range(ng)], axis=1))
            return thrice(split(thrice(left, whole, modes, NN)), left, modes, NT)

        square = jnp.zeros((LANES - modes, LANES), jnp.float32)

        def turned(value):
            return jnp.concatenate([value, square], 0).T[0:modes]

        def lay(forward, backward):
            rows[0:modes, :] = diagonals(backward, modes)
            rows[LANES : LANES + modes, :] = diagonals(forward, modes)

        if paired:

            @pl.when(straight)
            def _():
                both = projected()
                lay(both, turned(both))

            @pl.when(crossed)
            def _():
                both = projected()
                here, there = split(shapes[home, b]), split(shapes[away, b])
                across = thrice(split(thrice(here, split(mirror[b]), modes, NN)), there, modes, NT)
                lay(both + turned(across), turned(both) + across)

        else:
            both = projected()
            lay(both, turned(both))

        def slots_at(low, high):
            count = high - low
            return slots_of(
                lambda d: spread(rows, d, count) * first[b, d, low:high, :]
                + spread(rows, LANES + d, count) * second[b, d, low:high, :]
            )

        def place(g, low, score):
            score = score / denom[b, g, low : low + score.shape[0], :]
            at = slice(low // share, (low + score.shape[0]) // share)
            value = score.reshape(at.stop - at.start, share, depth_here)
            power[g, at] = value if b == 0 else power[g, at] + value

        early = slots_at(0, head)
        place(0, 0, form(b, 0, early))
        if b == nb - 1:
            for f in range(head // share):

                @pl.when(me != f * ng)
                def _():
                    part(jnp.int32(f), jnp.int32(0)).start()

        late = slots_at(head, ranges)
        if head < ranges:
            place(0, head, form(b, 0, late))
        every = [jnp.concatenate(pair, 0) for pair in zip(early, late)]
        for g in range(1, ng):
            place(g, 0, form(b, g, every))

    for j in range(devices - 1, 0, -1):
        f, g = flipped(j)

        @pl.when((f >= head // share) | (g > 0))
        def _():
            part(f, g).start()

    parts[me] = power[my_g, my_f]

    for k in range(1, ng):
        settle(modes_out.at[:, pl.ds(0, nb)], mode_send.at[k - 1])

    if paired:
        settle(pieces(nf - 1 + nf - span), send_sem.at[0])

        @pl.when(crossed)
        def _():
            settle(pieces(per - 1), send_sem.at[1])

        @pl.when(straight)
        def _():
            relay_copy().wait_send()

    else:
        settle(pieces(devices - 1), send_sem.at[0])

    settle(parts.at[pl.ds(0, devices - 1)], part_send)
    settle(parts.at[pl.ds(0, devices - 1)], part_recv)
    out_ref[...] = jnp.sum(parts[...], axis=0)


def solution(mesh):
    nf, ng = mesh.shape["freq"], mesh.shape["grid"]
    devices = nf * ng

    def per_device(cross_spectra, sensor_modes, source_modes, wavenumber, attenuation, mode_counts):
        two, bins, rows, cols = cross_spectra.shape
        bins_here, modes, _ = sensor_modes.shape
        depth_here = source_modes.shape[2]
        nb = bins_here // ng
        ranges = RANGES // nf * nf
        share = ranges // nf
        slots = modes // 2 + 3
        f32, bf16 = jnp.float32, jnp.bfloat16
        dma = pltpu.SemaphoreType.DMA
        operands = (
            cross_spectra, sensor_modes, source_modes, wavenumber, attenuation, mode_counts
        )
        return pl.pallas_call(
            functools.partial(kernel, nf, ng),
            out_shape=jax.ShapeDtypeStruct((share, depth_here), f32),
            in_specs=[pl.BlockSpec(memory_space=pltpu.HBM)] * 6,
            out_specs=pl.BlockSpec(memory_space=pltpu.VMEM),
            scratch_shapes=[
                pltpu.VMEM((2, bins_here, modes), f32),
                pltpu.SMEM((bins_here,), jnp.int32),
                pltpu.VMEM((two, bins, rows, cols), f32),
                pltpu.VMEM((nf, ng, nb, rows, cols), f32),
                pltpu.VMEM((nf, ng, nb, rows, cols), f32),
                pltpu.VMEM((ng, nb, nf * rows, cols), f32),
                pltpu.VMEM((nb, nf // ng * rows, cols), f32),
                pltpu.VMEM((nf // PLANES, nb, rows, cols), f32),
                pltpu.VMEM((2, bins_here, modes, cols), f32),
                pltpu.VMEM((ng, nb, LANES, cols), f32),
                pltpu.VMEM((ng, nb, 2 * modes, depth_here), f32),
                pltpu.VMEM((nb, modes // 2 + 1, ranges, LANES), f32),
                pltpu.VMEM((nb, modes // 2 + 1, ranges, LANES), f32),
                pltpu.VMEM((nb, ng, slots * LANES, depth_here), bf16),
                pltpu.VMEM((2 * LANES, LANES), f32),
                pltpu.VMEM((nb, ng, ranges, depth_here), f32),
                pltpu.VMEM((ng, nf, share, depth_here), f32),
                pltpu.VMEM((devices, share, depth_here), f32),
                pltpu.SemaphoreType.REGULAR((PLANES - 1,)),
                dma((2,)), dma, dma((2,)), dma((max(ng - 1, 1),)), dma((max(ng - 1, 1),)),
                dma((2,)), dma((2,)), dma, dma, dma, dma,
            ],
            compiler_params=pltpu.CompilerParams(
                collective_id=0, has_side_effects=True, vmem_limit_bytes=32 * 1024 * 1024
            ),
        )(*[pltpu.with_memory_space_constraint(x, pltpu.HBM) for x in operands])

    placed = (
        P(None, None, "freq", "grid"),
        P("freq", None, "grid"),
        P("freq", None, "grid"),
        P("freq", None),
        P("freq", None),
        P("freq"),
    )
    return jax.shard_map(
        per_device, mesh=mesh, in_specs=placed, out_specs=P("freq", "grid"), check_vma=False
    )
```
